32 devices in a mesh: dp: 1 (over z), tp: 4 (over y), ep: 8 (over x, core).
Axes of the slice: x: 4, y: 4, z: 1, core: 2. Of those that a mesh axis runs over, the one named last changes fastest.
The devices are a block of a 4x4x8 slice.
Arguments:
- hidden_in: bfloat16 [128, 256, 768], P(('dp', 'ep'), 'tp')
- ln_attn: float32 [2, 768], replicated
- ln_ffn: float32 [2, 768], replicated
- w_query: bfloat16 [2, 768, 768], P(None, None, 'tp')
- w_key: bfloat16 [2, 768, 768], P(None, None, 'tp')
- w_value: bfloat16 [2, 768, 768], P(None, None, 'tp')
- w_out: bfloat16 [2, 768, 768], P(None, 'tp')
- bias_table: float32 [2, 12, 32], P(None, 'tp')
- w_gate: bfloat16 [768, 3072], P(None, 'tp')
- w_up: bfloat16 [768, 3072], P(None, 'tp')
- w_down: bfloat16 [3072, 768], P('tp')
- w_router: float32 [768, 128], replicated
- expert_in: bfloat16 [128, 768, 3072], P(('tp', 'ep'))
- expert_out: bfloat16 [128, 3072, 768], P(('tp', 'ep'))
- expert_ids: int32 [128, 256, 2], P(('dp', 'ep'), 'tp')
Outputs:
- output 1: bfloat16 [128, 256, 768], P(('dp', 'ep'), 'tp')
- output 2: bfloat16 [2, 128, 12, 256, 64], P(None, ('dp', 'ep'), 'tp')
- output 3: bfloat16 [2, 128, 12, 256, 64], P(None, ('dp', 'ep'), 'tp')
All inputs are finite; a program needn't handle non-finite values.
Results may differ from the reference program's by a relative error of at most 0.0120554.
Values are sent between devices in bfloat16 or wider.
A program may use at most 768 MiB of HBM per device.

```python
import jax
import jax.numpy as jnp
from jax import lax

D_MODEL = 768
NUM_HEADS = 12
HEAD_DIM = 64
FF_DIM = 3072
NUM_EXPERTS = 128
EP_SIZE = 8
TP_SIZE = 4
BATCH = 128
SEQ_LEN = 256
NUM_BUCKETS = 32
EXACT_BUCKETS = 16

THRESHOLDS = (18, 20, 23, 26, 30, 34, 39, 45, 51, 58, 66, 76, 86, 98, 112)
EPSILON = 1e-6
INNER = NUM_HEADS * HEAD_DIM
LOCAL_BATCH = BATCH // EP_SIZE
LOCAL_SEQ = SEQ_LEN // TP_SIZE
LOCAL_TOKENS = LOCAL_BATCH * LOCAL_SEQ
NUM_GROUPS = EP_SIZE * TP_SIZE
CAPACITY = 4 * LOCAL_TOKENS // NUM_EXPERTS


def draw_ids(id_key):
    coin_key, hot_key, start_key, uniform_key, second_key = jax.random.split(id_key, 5)
    id_shape = (BATCH, SEQ_LEN)
    hot_width = max(NUM_EXPERTS // 8, 1)
    hot_start = jax.random.randint(start_key, (), 0, NUM_EXPERTS)
    hot_pick = (hot_start + jax.random.randint(hot_key, id_shape, 0, hot_width)) % NUM_EXPERTS
    uniform_pick = jax.random.randint(uniform_key, id_shape, 0, NUM_EXPERTS)
    coin_flip = jax.random.randint(coin_key, id_shape, 0, 4)
    first_pick = jnp.where(coin_flip == 0, hot_pick, uniform_pick)
    flat_pos = jnp.arange(BATCH * SEQ_LEN).reshape(id_shape)
    first_pick = jnp.where(flat_pos < NUM_EXPERTS, flat_pos, first_pick)
    second_pick = (first_pick + 1 + jax.random.randint(second_key, id_shape, 0, NUM_EXPERTS - 1)) % NUM_EXPERTS
    return jnp.stack([first_pick, second_pick], axis=-1).astype(jnp.int32)


def setup_inputs(seed: int = 0, part: int = 0) -> dict:
    keys_all = jax.random.split(jax.random.key(seed), 16)
    part_key = jax.random.fold_in(keys_all[0], part)
    act_key, id_key = jax.random.split(part_key)

    def normal(sub_key, dim_tuple, scale_by):
        return jax.random.normal(sub_key, dim_tuple, jnp.float32) * scale_by

    return {
        'hidden_in': normal(act_key, (BATCH, SEQ_LEN, D_MODEL), 1.0).astype(jnp.bfloat16),
        'ln_attn': jax.random.uniform(keys_all[1], (2, D_MODEL), jnp.float32, 0.5, 1.5),
        'ln_ffn': jax.random.uniform(keys_all[2], (2, D_MODEL), jnp.float32, 0.5, 1.5),
        'w_query': normal(keys_all[3], (2, D_MODEL, INNER), D_MODEL ** -0.5).astype(jnp.bfloat16),
        'w_key': normal(keys_all[4], (2, D_MODEL, INNER), D_MODEL ** -0.5).astype(jnp.bfloat16),
        'w_value': normal(keys_all[5], (2, D_MODEL, INNER), D_MODEL ** -0.5).astype(jnp.bfloat16),
        'w_out': normal(keys_all[6], (2, INNER, D_MODEL), INNER ** -0.5).astype(jnp.bfloat16),
        'bias_table': normal(keys_all[7], (2, NUM_HEADS, NUM_BUCKETS), 1.5),
        'w_gate': normal(keys_all[8], (D_MODEL, FF_DIM), D_MODEL ** -0.5).astype(jnp.bfloat16),
        'w_up': normal(keys_all[9], (D_MODEL, FF_DIM), D_MODEL ** -0.5).astype(jnp.bfloat16),
        'w_down': normal(keys_all[10], (FF_DIM, D_MODEL), FF_DIM ** -0.5).astype(jnp.bfloat16),
        'w_router': normal(keys_all[11], (D_MODEL, NUM_EXPERTS), D_MODEL ** -0.5),
        'expert_in': normal(keys_all[12], (NUM_EXPERTS, D_MODEL, FF_DIM), D_MODEL ** -0.5).astype(jnp.bfloat16),
        'expert_out': normal(keys_all[13], (NUM_EXPERTS, FF_DIM, D_MODEL), FF_DIM ** -0.5).astype(jnp.bfloat16),
        'expert_ids': draw_ids(id_key),
    }


def bucket_of(rel_pos):
    bucket_idx = jnp.minimum(rel_pos, EXACT_BUCKETS)
    for threshold in THRESHOLDS:
        bucket_idx = bucket_idx + (rel_pos >= threshold).astype(jnp.int32)
    return bucket_idx


def rms_norm(rows_in, ln_scale):
    wide_rows = rows_in.astype(jnp.float32)
    inv_rms = lax.rsqrt(jnp.mean(wide_rows * wide_rows, axis=-1, keepdims=True) + EPSILON)
    return (wide_rows * inv_rms * ln_scale).astype(jnp.bfloat16)


def causal_bias(bias_rows):
    positions = jnp.arange(SEQ_LEN)
    rel_pos = positions[:, None] - positions[None, :]
    bias_full = jnp.take(bias_rows, bucket_of(jnp.maximum(rel_pos, 0)), axis=1)
    return jnp.where(rel_pos[None] >= 0, bias_full, -jnp.inf)


def attention(hidden, ln_scale, w_query, w_key, w_value, w_out, bias_rows):
    normed = rms_norm(hidden, ln_scale).reshape(BATCH * SEQ_LEN, D_MODEL)

    def project(weight):
        projected = jnp.dot(normed, weight, preferred_element_type=jnp.float32)
        return projected.astype(jnp.bfloat16).reshape(BATCH, SEQ_LEN, NUM_HEADS, HEAD_DIM)

    queries = project(w_query)
    keys_full = project(w_key)
    values_full = project(w_value)
    bias_full = causal_bias(bias_rows)

    def one_sequence(operands):
        query_seq, key_seq, value_seq = operands
        scores = jnp.einsum('qhd,khd->hqk', query_seq.astype(jnp.float32), key_seq.astype(jnp.float32))
        scores = scores * (HEAD_DIM ** -0.5) + bias_full
        attn_probs = jax.nn.softmax(scores, axis=-1).astype(jnp.bfloat16)
        context = jnp.einsum('hqk,khd->qhd', attn_probs.astype(jnp.float32), value_seq.astype(jnp.float32))
        return context.astype(jnp.bfloat16)

    context = lax.map(one_sequence, (queries, keys_full, values_full)).reshape(BATCH * SEQ_LEN, INNER)
    attn_out = jnp.dot(context, w_out, preferred_element_type=jnp.float32).reshape(BATCH, SEQ_LEN, D_MODEL)
    new_hidden = (hidden.astype(jnp.float32) + attn_out).astype(jnp.bfloat16)
    return new_hidden, jnp.swapaxes(keys_full, 1, 2), jnp.swapaxes(values_full, 1, 2)


def dense_ffn(hidden, ln_scale, w_gate, w_up, w_down):
    normed = rms_norm(hidden, ln_scale).reshape(BATCH * SEQ_LEN, D_MODEL)
    gate_pre = jnp.dot(normed, w_gate, preferred_element_type=jnp.float32)
    up_pre = jnp.dot(normed, w_up, preferred_element_type=jnp.float32)
    ffn_hidden = (jax.nn.gelu(gate_pre) * up_pre).astype(jnp.bfloat16)
    ffn_out = jnp.dot(ffn_hidden, w_down, preferred_element_type=jnp.float32).reshape(BATCH, SEQ_LEN, D_MODEL)
    return (hidden.astype(jnp.float32) + ffn_out).astype(jnp.bfloat16)


def to_groups(array_in):
    tail_dims = array_in.shape[2:]
    split_view = array_in.reshape((EP_SIZE, LOCAL_BATCH, TP_SIZE, LOCAL_SEQ) + tail_dims)
    return jnp.swapaxes(split_view, 1, 2).reshape((NUM_GROUPS, LOCAL_TOKENS) + tail_dims)


def from_groups(array_in):
    tail_dims = array_in.shape[2:]
    split_view = array_in.reshape((EP_SIZE, TP_SIZE, LOCAL_BATCH, LOCAL_SEQ) + tail_dims)
    return jnp.swapaxes(split_view, 1, 2).reshape((BATCH, SEQ_LEN) + tail_dims)


def slot_table(choices):
    experts = jnp.arange(NUM_EXPERTS, dtype=jnp.int32)
    first_hot = (choices[..., 0:1] == experts).astype(jnp.int32)
    second_hot = (choices[..., 1:2] == experts).astype(jnp.int32)
    first_pos = jnp.sum((jnp.cumsum(first_hot, axis=-2) - 1) * first_hot, axis=-1)
    second_base = jnp.cumsum(second_hot, axis=-2) - 1 + jnp.sum(first_hot, axis=-2, keepdims=True)
    second_pos = jnp.sum(second_base * second_hot, axis=-1)
    position = jnp.stack([first_pos, second_pos], axis=-1)
    return jnp.where(position < CAPACITY, choices * CAPACITY + position, NUM_EXPERTS * CAPACITY)


def dispatch(group_rows, slot_ids):
    buffer_rows = jnp.zeros((NUM_EXPERTS * CAPACITY + 1, D_MODEL), jnp.bfloat16)
    buffer_rows = buffer_rows.at[slot_ids[:, 0]].set(group_rows).at[slot_ids[:, 1]].set(group_rows)
    return buffer_rows[:-1]


def run_expert(operands):
    rows_in, weight_in, weight_out = operands
    expert_hidden = jax.nn.gelu(jnp.dot(rows_in, weight_in, preferred_element_type=jnp.float32)).astype(jnp.bfloat16)
    return jnp.dot(expert_hidden, weight_out, preferred_element_type=jnp.float32).astype(jnp.bfloat16)


def gather_rows(table_rows, slot_ids):
    return jnp.take(table_rows, slot_ids, axis=0)


def moe_layer(hidden, ln_scale, w_router, expert_in, expert_out, expert_ids):
    tok_rows = to_groups(rms_norm(hidden, ln_scale))
    choices = to_groups(expert_ids)
    logits = jnp.einsum('gnd,de->gne', tok_rows.astype(jnp.float32), w_router)
    router_probs = jax.nn.softmax(logits, axis=-1)
    picked = jnp.take_along_axis(router_probs, choices, axis=-1)
    gate_weights = picked / jnp.sum(picked, axis=-1, keepdims=True)
    slot_ids = slot_table(choices)
    buffers = jax.vmap(dispatch)(tok_rows, slot_ids)
    per_expert = jnp.swapaxes(buffers.reshape(NUM_GROUPS, NUM_EXPERTS, CAPACITY, D_MODEL), 0, 1)
    per_expert = per_expert.reshape(NUM_EXPERTS, NUM_GROUPS * CAPACITY, D_MODEL)
    expert_result = lax.map(run_expert, (per_expert, expert_in, expert_out))
    returned = jnp.swapaxes(expert_result.reshape(NUM_EXPERTS, NUM_GROUPS, CAPACITY, D_MODEL), 0, 1)
    returned = returned.reshape(NUM_GROUPS, NUM_EXPERTS * CAPACITY, D_MODEL)
    padded = jnp.concatenate([returned, jnp.zeros((NUM_GROUPS, 1, D_MODEL), jnp.bfloat16)], axis=1)
    gathered_out = jax.vmap(gather_rows)(padded, slot_ids)
    moe_sum = jnp.sum(gate_weights[..., None] * gathered_out.astype(jnp.float32), axis=2)
    return (hidden.astype(jnp.float32) + from_groups(moe_sum)).astype(jnp.bfloat16)


def reference(hidden_in, ln_attn, ln_ffn, w_query, w_key, w_value, w_out, bias_table, w_gate, w_up, w_down, w_router, expert_in, expert_out, expert_ids):
    hidden, keys_zero, values_zero = attention(hidden_in, ln_attn[0], w_query[0], w_key[0], w_value[0], w_out[0], bias_table[0])
    hidden = dense_ffn(hidden, ln_ffn[0], w_gate, w_up, w_down)
    hidden, keys_one, values_one = attention(hidden, ln_attn[1], w_query[1], w_key[1], w_value[1], w_out[1], bias_table[1])
    hidden = moe_layer(hidden, ln_ffn[1], w_router, expert_in, expert_out, expert_ids)
    return hidden, jnp.stack([keys_zero, keys_one]), jnp.stack([values_zero, values_one])
```

```python
import functools

import jax
import jax.numpy as jnp
from jax import lax
from jax.experimental import pallas as pl
from jax.experimental.pallas import tpu as pltpu
from jax.sharding import PartitionSpec as P

EXACT_BUCKETS = 16
THRESHOLDS = (18, 20, 23, 26, 30, 34, 39, 45, 51, 58, 66, 76, 86, 98, 112)
EPSILON = 1e-6
GROUP = ('tp', 'ep')
MESH = pl.DeviceIdType.MESH


def rms_norm(rows_in, ln_scale):
    wide_rows = rows_in.astype(jnp.float32)
    inv_rms = lax.rsqrt(jnp.mean(wide_rows * wide_rows, axis=-1, keepdims=True) + EPSILON)
    return (wide_rows * inv_rms * ln_scale).astype(jnp.bfloat16)


def tp_exchange_permutes(blocks, tp):
    me = lax.axis_index('tp')
    out = lax.dynamic_update_index_in_dim(jnp.zeros_like(blocks), lax.dynamic_index_in_dim(blocks, me, 0), me, 0)
    for step in range(1, tp):
        block = lax.dynamic_index_in_dim(blocks, (me + step) % tp, 0)
        got = lax.ppermute(block, 'tp', [(i, (i + step) % tp) for i in range(tp)])
        out = lax.dynamic_update_index_in_dim(out, got, (me + tp - step) % tp, 0)
    return out


def gather_kernel(tp, ep, num_blocks, direct, hidden_ref, table_ref, *refs):
    sources, refs = refs[:num_blocks], refs[num_blocks:]
    seqs_ref, relay_ref, tables_ref, refs = refs[0], refs[1], refs[2], refs[3:]
    gathered, refs = refs[:num_blocks], refs[num_blocks:]
    stage_ref, stage_hidden_ref, send_sem, recv_sem, in_sem, out_sem = refs
    me_tp, me_ep = lax.axis_index('tp'), lax.axis_index('ep')
    right, left, across = lax.rem(me_tp + 1, tp), lax.rem(me_tp + tp - 1, tp), lax.rem(me_tp + 2, tp)
    east, west, beyond = lax.rem(me_ep + 2, ep), lax.rem(me_ep + ep - 2, ep), lax.rem(me_ep + 4, ep)
    partner = me_ep + 1 - 2 * lax.rem(me_ep, 2)
    peers = ({'tp': right}, {'tp': left}, {'tp': across}, {'ep': east}, {'ep': west}, {'ep': partner})
    to_right, to_left, to_across, to_east, to_west, to_partner = peers

    barrier = pltpu.get_barrier_semaphore()
    for peer in peers:
        pl.semaphore_signal(barrier, inc=1, device_id=peer, device_id_type=MESH)
    pl.semaphore_wait(barrier, len(peers))

    copies = []

    def send(source, target, peer):
        index = len(copies)
        copy = pltpu.make_async_remote_copy(src_ref=source, dst_ref=target, send_sem=send_sem.at[index], recv_sem=recv_sem.at[index],
                                            device_id=peer, device_id_type=MESH)
        copy.start()
        copies.append(copy)
        return copy

    rows = sources[0].shape[1]
    halves = (slice(0, rows // 2), slice(rows // 2, rows))
    sliced = [block for block in range(num_blocks) if block != direct]
    locals_in = [pltpu.make_async_copy(sources[block], stage_ref.at[block], in_sem.at[block]) for block in range(num_blocks)]
    locals_in.append(pltpu.make_async_copy(hidden_ref.at[me_tp], stage_hidden_ref, in_sem.at[num_blocks]))

    first = {}
    for block in sliced:
        first[block] = [send(sources[block].at[me_ep], gathered[block].at[me_tp, me_ep], peer) for peer in (to_right, to_left)]
    tables = [send(table_ref, tables_ref.at[me_tp], peer) for peer in (to_right, to_left, to_across)]
    for copy in locals_in:
        copy.start()
    tables_ref[me_tp] = table_ref[...]
    part = hidden_ref.shape[1] // 2
    relays = [send(hidden_ref.at[across, 0:part], relay_ref.at[0], to_right), send(hidden_ref.at[across, part:2 * part], relay_ref.at[1], to_left)]

    def share(block, group, index, span=None):
        ref = gathered[block]
        return ref.at[group, index] if span is None else ref.at[group, index, span]

    received = []
    forward, sideways = {}, {}
    for block in sliced:
        first[block][0].wait_recv()
        forward[block] = [send(share(block, left, me_ep, halves[0]), share(block, left, me_ep, halves[0]), to_right)]
        sideways[block] = {}
        for group, name in ((left, 'left'), (right, 'right')):
            if name == 'right':
                first[block][1].wait_recv()
                forward[block].append(send(share(block, right, me_ep, halves[1]), share(block, right, me_ep, halves[1]), to_left))
            whole = share(block, group, me_ep)
            sideways[block][name] = [send(whole, whole, to_east), send(whole, whole, to_west)]
            received.append(send(whole, whole, to_partner))
    core_half = ep // 2
    base = lax.rem(me_ep, 2) * core_half
    near = pl.ds(base, core_half)
    direct_first = [send(sources[direct].at[near], gathered[direct].at[me_tp, near], peer) for peer in (to_right, to_left)]
    swaps = [send(hidden_ref.at[right], seqs_ref.at[:, me_tp], to_right), send(hidden_ref.at[left], seqs_ref.at[:, me_tp], to_left)]
    for block in sliced:
        for copy in forward[block]:
            copy.wait_recv()
        whole = share(block, across, me_ep)
        sideways[block]['across'] = [send(whole, whole, to_east), send(whole, whole, to_west)]
        received.append(send(whole, whole, to_partner))
    for copy in relays:
        copy.wait_recv()
    swaps.append(send(relay_ref.at[0], seqs_ref.at[0:part, left], to_right))
    swaps.append(send(relay_ref.at[1], seqs_ref.at[part:2 * part, right], to_left))
    for copy in locals_in:
        copy.wait()
    locals_out = [pltpu.make_async_copy(stage_ref.at[block], gathered[block].at[me_tp], out_sem.at[block]) for block in range(num_blocks)]
    locals_out.append(pltpu.make_async_copy(stage_hidden_ref, seqs_ref.at[:, me_tp], out_sem.at[num_blocks]))
    for copy in locals_out:
        copy.start()

    def direct_ring():
        for copy in direct_first:
            copy.wait_recv()
        lower, upper = pl.ds(base, core_half // 2), pl.ds(base + core_half // 2, core_half // 2)
        last = [send(gathered[direct].at[left, lower], gathered[direct].at[left, lower], to_right),
                send(gathered[direct].at[right, upper], gathered[direct].at[right, upper], to_left)]
        for group in (left, right):
            received.append(send(gathered[direct].at[group, near], gathered[direct].at[group, near], to_partner))
        return last

    direct_last = None
    final = []
    groups = {'left': left, 'right': right, 'across': across}
    for count, block in enumerate(sliced):
        for name in ('left', 'right', 'across'):
            group = groups[name]
            sideways[block][name][0].wait_recv()
            pair = [send(share(block, group, west, halves[0]), share(block, group, west, halves[0]), to_east)]
            whole = share(block, group, west)
            received.append(send(whole, whole, to_partner))
            sideways[block][name][1].wait_recv()
            pair.append(send(share(block, group, east, halves[1]), share(block, group, east, halves[1]), to_west))
            whole = share(block, group, east)
            received.append(send(whole, whole, to_partner))
            final.append((block, group, pair))
        if count == 1:
            direct_last = direct_ring()
    for block, group, pair in final:
        for copy in pair:
            copy.wait_recv()
        whole = share(block, group, beyond)
        received.append(send(whole, whole, to_partner))
    for copy in direct_last:
        copy.wait_recv()
    whole = gathered[direct].at[across, near]
    received.append(send(whole, whole, to_partner))
    for copy in tables + swaps + received:
        copy.wait_recv()
    for copy in copies:
        copy.wait_send()
    for copy in locals_out:
        copy.wait()


def gather_all(hidden_in, table, blocks, direct, tp, ep):
    num_blocks = len(blocks)
    batch, local_seq, d_model = hidden_in.shape
    seqs = batch // tp
    hidden_view = hidden_in.reshape(tp, seqs, local_seq, d_model)
    views = [block.reshape(ep, block.shape[0] // ep, block.shape[1]) for block in blocks]
    any_spec = pl.BlockSpec(memory_space=pl.ANY)
    vmem_spec = pl.BlockSpec(memory_space=pltpu.VMEM)
    copies = 28 * (num_blocks - 1) + 7 + 9
    results = pl.pallas_call(
        functools.partial(gather_kernel, tp, ep, num_blocks, direct),
        in_specs=[any_spec, vmem_spec] + [any_spec] * num_blocks,
        out_specs=[any_spec, any_spec, vmem_spec] + [any_spec] * num_blocks,
        out_shape=[jax.ShapeDtypeStruct((seqs, tp, local_seq, d_model), hidden_in.dtype),
                   jax.ShapeDtypeStruct((2, seqs // 2, local_seq, d_model), hidden_in.dtype),
                   jax.ShapeDtypeStruct((tp,) + table.shape, table.dtype)]
        + [jax.ShapeDtypeStruct((tp,) + view.shape, view.dtype) for view in views],
        scratch_shapes=[pltpu.VMEM((num_blocks,) + views[0].shape, views[0].dtype), pltpu.VMEM((seqs, local_seq, d_model), hidden_in.dtype),
                        pltpu.SemaphoreType.DMA((copies,)), pltpu.SemaphoreType.DMA((copies,)),
                        pltpu.SemaphoreType.DMA((num_blocks + 1,)), pltpu.SemaphoreType.DMA((num_blocks + 1,))],
        compiler_params=pltpu.CompilerParams(collective_id=0, has_side_effects=True),
        name='gather_all',
    )(hidden_view, table, *views)
    hidden = results[0].reshape(seqs, tp * local_seq, d_model)
    tables = jnp.swapaxes(results[2], 0, 1).reshape(table.shape[0], -1, table.shape[2])
    return hidden, tables, [block.reshape(tp, -1, d_model) for block in results[3:]]


def attention_kernel(tp, hidden_ref, ln_ref, w_ref, table_ref, out_ref, keys_ref, values_ref, bias_ref, q_ref, kt_ref, ctx_ref, w_out_ref):
    seq_len, d_model = hidden_ref.shape[1], hidden_ref.shape[2]
    num_heads = table_ref.shape[0]
    head_dim = d_model // num_heads
    half = seq_len // 2
    width = d_model // tp
    starts = tuple(range(EXACT_BUCKETS + 1)) + THRESHOLDS

    @pl.when(pl.program_id(0) == 0)
    def _():
        def one_head(head, carry):
            for block in range(2):
                key_pos = lax.broadcasted_iota(jnp.int32, (half, half), 0)
                query_pos = lax.broadcasted_iota(jnp.int32, (half, half), 1) + block * half
                rel_pos = query_pos - key_pos
                bias = jnp.full((half, half), -jnp.inf, jnp.float32)
                for bucket, start in enumerate(starts):
                    bias = jnp.where(rel_pos >= start, table_ref[head, bucket], bias)
                bias_ref[head, :, block * half:(block + 1) * half] = bias
            return carry

        lax.fori_loop(0, num_heads, one_head, 0)
        for part in range(tp):
            w_out_ref[part * width:(part + 1) * width] = w_ref[part, 3 * width:]

    rows = hidden_ref[0].astype(jnp.float32)
    inv_rms = lax.rsqrt(jnp.mean(rows * rows, axis=-1, keepdims=True) + EPSILON)
    normed = (rows * inv_rms * ln_ref[...]).astype(jnp.bfloat16)
    nt = (((1,), (1,)), ((), ()))
    for part in range(tp):
        take = slice(part * width, (part + 1) * width)
        qkv = lax.dot_general(w_ref[part, :3 * width], normed, nt, preferred_element_type=jnp.float32).astype(jnp.bfloat16)
        q_ref[take] = qkv[:width]
        keys_ref[part, 0] = qkv[width:2 * width]
        values_ref[part, 0] = qkv[2 * width:]
        kt_ref[take] = qkv[width:2 * width]

    local_heads = num_heads // tp
    zeros = jnp.zeros((head_dim, seq_len), jnp.bfloat16)
    for head in range(num_heads):
        pair = slice((head // 2) * 2 * head_dim, (head // 2 + 1) * 2 * head_dim)
        q_head = q_ref[head * head_dim:(head + 1) * head_dim]
        q_pair = jnp.concatenate([q_head, zeros] if head % 2 == 0 else [zeros, q_head], axis=0)
        scores = jnp.dot(kt_ref[pair].T, q_pair, preferred_element_type=jnp.float32)
        value = values_ref[head // local_heads, 0, (head % local_heads) * head_dim:(head % local_heads + 1) * head_dim]
        near, far = bias_ref[head, :, :half], bias_ref[head, :, half:]
        scale = head_dim ** -0.5
        first = scores[:half, :half] * scale + near
        first = jnp.exp(first - jnp.max(first, axis=0, keepdims=True))
        probs = (first / jnp.sum(first, axis=0, keepdims=True)).astype(jnp.bfloat16)
        ctx_first = jnp.dot(value[:, :half], probs, preferred_element_type=jnp.float32)
        low = scores[:half, half:] * scale + far
        high = scores[half:, half:] * scale + near
        top = jnp.maximum(jnp.max(low, axis=0, keepdims=True), jnp.max(high, axis=0, keepdims=True))
        low, high = jnp.exp(low - top), jnp.exp(high - top)
        total = jnp.sum(low, axis=0, keepdims=True) + jnp.sum(high, axis=0, keepdims=True)
        probs = jnp.concatenate([(low / total).astype(jnp.bfloat16), (high / total).astype(jnp.bfloat16)], axis=0)
        ctx_second = jnp.dot(value, probs, preferred_element_type=jnp.float32)
        ctx = jnp.concatenate([ctx_first, ctx_second], axis=1)
        ctx_ref[head * head_dim:(head + 1) * head_dim] = ctx.astype(jnp.bfloat16)
    attn_out = jnp.dot(ctx_ref[...].T, w_out_ref[...], preferred_element_type=jnp.float32)
    out_ref[0] = (rows + attn_out).astype(jnp.bfloat16)


def attention(hidden, ln_scale, packed, table, tp):
    seqs, seq_len, d_model = hidden.shape
    num_heads = table.shape[0]
    width = d_model // tp
    seq_block = pl.BlockSpec((1, seq_len, d_model), lambda s: (s, 0, 0))
    cache_block = pl.BlockSpec((tp, 1, width, seq_len), lambda s: (0, s, 0, 0))
    cache = jax.ShapeDtypeStruct((tp, seqs, width, seq_len), jnp.bfloat16)
    flops = 2 * seqs * seq_len * d_model * (5 * d_model + 3 * seq_len)
    return pl.pallas_call(
        functools.partial(attention_kernel, tp),
        grid=(seqs,),
        in_specs=[seq_block, pl.BlockSpec((1, d_model), lambda s: (0, 0)), pl.BlockSpec((tp, d_model, d_model), lambda s: (0, 0, 0)),
                  pl.BlockSpec(memory_space=pltpu.SMEM)],
        out_specs=[seq_block, cache_block, cache_block],
        out_shape=[jax.ShapeDtypeStruct(hidden.shape, hidden.dtype), cache, cache],
        scratch_shapes=[pltpu.VMEM((num_heads, seq_len // 2, seq_len), jnp.float32), pltpu.VMEM((d_model, seq_len), jnp.bfloat16),
                        pltpu.VMEM((d_model, seq_len), jnp.bfloat16), pltpu.VMEM((d_model, seq_len), jnp.bfloat16),
                        pltpu.VMEM((d_model, d_model), jnp.bfloat16)],
        compiler_params=pltpu.CompilerParams(dimension_semantics=('arbitrary',), vmem_limit_bytes=40 * 1024 * 1024),
        cost_estimate=pl.CostEstimate(flops=flops, bytes_accessed=2 * (hidden.size * 4 + packed.size), transcendentals=0),
        name='attention',
    )(hidden, ln_scale[None], packed, table)


def dense_ffn(hidden, ln_scale, gate, up, down):
    normed = rms_norm(hidden, ln_scale)
    gate_pre = jnp.einsum('std,gdf->stgf', normed, gate, preferred_element_type=jnp.float32)
    up_pre = jnp.einsum('std,gdf->stgf', normed, up, preferred_element_type=jnp.float32)
    ffn_hidden = (jax.nn.gelu(gate_pre) * up_pre).astype(jnp.bfloat16)
    ffn_out = jnp.einsum('stgf,gfd->std', ffn_hidden, down, preferred_element_type=jnp.float32)
    return (hidden.astype(jnp.float32) + ffn_out).astype(jnp.bfloat16)


def slot_table(choices, num_experts):
    experts = jnp.arange(num_experts, dtype=jnp.int32)
    first_hot = (choices[..., 0:1] == experts).astype(jnp.int32)
    second_hot = (choices[..., 1:2] == experts).astype(jnp.int32)
    first_pos = jnp.sum((jnp.cumsum(first_hot, axis=-2) - 1) * first_hot, axis=-1)
    second_base = jnp.cumsum(second_hot, axis=-2) - 1 + jnp.sum(first_hot, axis=-2, keepdims=True)
    second_pos = jnp.sum(second_base * second_hot, axis=-1)
    return jnp.stack([first_pos, second_pos], axis=-1)


def moe_block(hidden, ln_scale, w_router, expert_in, expert_out, expert_ids, caches):
    local_batch, local_seq, d_model = hidden.shape
    tokens = local_batch * local_seq
    num_experts = w_router.shape[1]
    local_experts = expert_in.shape[0]
    groups = num_experts // local_experts
    capacity = 4 * tokens // num_experts
    choices = expert_ids.reshape(tokens, 2)
    position = slot_table(choices, num_experts)
    slot_ids = jnp.where(position < capacity, choices * capacity + position, -1)
    columns = jnp.arange(num_experts * capacity, dtype=jnp.int32)
    select = (slot_ids[:, :, None] == columns).astype(jnp.bfloat16)

    normed = rms_norm(hidden, ln_scale).reshape(tokens, d_model)
    dispatched = jnp.einsum('ncs,nd->sd', select, normed, preferred_element_type=jnp.float32).astype(jnp.bfloat16)
    dispatched = dispatched.reshape(groups, local_experts, capacity, d_model)
    received = lax.all_to_all(dispatched, GROUP, 0, 2, tiled=True)
    expert_rows = received.reshape(local_experts, groups * capacity, d_model)

    logits = jnp.dot(normed.astype(jnp.float32), w_router, precision=lax.Precision.HIGHEST)
    router_probs = jax.nn.softmax(logits, axis=-1)
    experts = jnp.arange(num_experts, dtype=jnp.int32)
    picked = jnp.sum(jnp.where(choices[:, :, None] == experts, router_probs[:, None, :], 0.0), axis=-1)
    gate_weights = picked / jnp.sum(picked, axis=-1, keepdims=True)

    expert_hidden = jnp.einsum('erd,edf->erf', expert_rows, expert_in, preferred_element_type=jnp.float32)
    expert_hidden = jax.nn.gelu(expert_hidden).astype(jnp.bfloat16)
    expert_result = jnp.einsum('erf,efd->erd', expert_hidden, expert_out, preferred_element_type=jnp.float32).astype(jnp.bfloat16)
    expert_result, *caches = lax.optimization_barrier((expert_result, *caches))
    expert_result = expert_result.reshape(1, local_experts, groups * capacity, d_model)
    returned = lax.all_to_all(expert_result, GROUP, 2, 0, tiled=True)
    returned = returned.reshape(num_experts * capacity, d_model)
    gathered_out = jnp.einsum('ncs,sd->ncd', select, returned, preferred_element_type=jnp.float32)
    moe_sum = jnp.sum(gate_weights[:, :, None] * gathered_out, axis=1).reshape(local_batch, local_seq, d_model)
    return (hidden.astype(jnp.float32) + moe_sum).astype(jnp.bfloat16), *caches


def solution(mesh):
    tp, ep = mesh.shape['tp'], mesh.shape['ep']
    act_spec = P(('dp', 'ep'), 'tp', None)
    col_spec = P(None, None, 'tp')
    row_spec = P(None, 'tp', None)
    expert_spec = P(('tp', 'ep'), None, None)
    cache_spec = P(None, ('dp', 'ep'), 'tp', None, None)
    in_specs = (act_spec, P(), P(), col_spec, col_spec, col_spec, row_spec, row_spec,
                P(None, 'tp'), P(None, 'tp'), P('tp', None), P(), expert_spec, expert_spec, act_spec)

    def to_owner(blocks, local_heads):
        got = tp_exchange_permutes(blocks, tp)
        return jnp.swapaxes(got.reshape(got.shape[0] * got.shape[1], local_heads, -1, got.shape[3]), 2, 3)

    def device_fn(hidden_in, ln_attn, ln_ffn, w_query, w_key, w_value, w_out, bias_table, w_gate, w_up, w_down, w_router, expert_in, expert_out, expert_ids):
        def packed(layer):
            parts = [jnp.swapaxes(w[layer], 0, 1) for w in (w_query, w_key, w_value)] + [w_out[layer]]
            return jnp.concatenate(parts, axis=0)

        local_heads = bias_table.shape[1]
        blocks = [packed(0), w_up, w_down, packed(1), w_gate]
        hidden, tables, (attn_zero, up, down, attn_one, gate) = gather_all(hidden_in, bias_table, blocks, len(blocks) - 1, tp, ep)
        hidden, keys_zero, values_zero = attention(hidden, ln_attn[0], attn_zero, tables[0], tp)
        keys_zero, values_zero = to_owner(keys_zero, local_heads), to_owner(values_zero, local_heads)
        hidden = dense_ffn(hidden, ln_ffn[0], gate, up, down)
        hidden, keys_one, values_one = attention(hidden, ln_attn[1], attn_one, tables[1], tp)
        hidden, keys_zero, values_zero = lax.optimization_barrier((hidden, keys_zero, values_zero))
        keys_one, values_one = to_owner(keys_one, local_heads), to_owner(values_one, local_heads)
        hidden = lax.all_to_all(hidden, 'tp', 1, 0, tiled=True)
        hidden, keys_one, values_one = moe_block(hidden, ln_ffn[1], w_router, expert_in, expert_out, expert_ids, (keys_one, values_one))
        keys, values = jnp.stack([keys_zero, keys_one]), jnp.stack([values_zero, values_one])
        return hidden, keys, values

    return jax.shard_map(device_fn, mesh=mesh, in_specs=in_specs, out_specs=(act_spec, cache_spec, cache_spec), check_vma=False)
```

```python
import functools

import jax
import jax.numpy as jnp
from jax import lax
from jax.experimental import pallas as pl
from jax.experimental.pallas import tpu as pltpu
from jax.sharding import PartitionSpec as P

EXACT_BUCKETS = 16
THRESHOLDS = (18, 20, 23, 26, 30, 34, 39, 45, 51, 58, 66, 76, 86, 98, 112)
EPSILON = 1e-6
GROUP = ('tp', 'ep')
MESH = pl.DeviceIdType.MESH


def rms_norm(rows_in, ln_scale):
    wide_rows = rows_in.astype(jnp.float32)
    inv_rms = lax.rsqrt(jnp.mean(wide_rows * wide_rows, axis=-1, keepdims=True) + EPSILON)
    return (wide_rows * inv_rms * ln_scale).astype(jnp.bfloat16)


def tp_exchange_permutes(blocks, tp):
    me = lax.axis_index('tp')
    out = lax.dynamic_update_index_in_dim(jnp.zeros_like(blocks), lax.dynamic_index_in_dim(blocks, me, 0), me, 0)
    for step in range(1, tp):
        block = lax.dynamic_index_in_dim(blocks, (me + step) % tp, 0)
        got = lax.ppermute(block, 'tp', [(i, (i + step) % tp) for i in range(tp)])
        out = lax.dynamic_update_index_in_dim(out, got, (me + tp - step) % tp, 0)
    return out


def gather_kernel(tp, ep, num_blocks, direct, hidden_ref, table_ref, *refs):
    sources, refs = refs[:num_blocks], refs[num_blocks:]
    seqs_ref, relay_ref, tables_ref, refs = refs[0], refs[1], refs[2], refs[3:]
    gathered, refs = refs[:num_blocks], refs[num_blocks:]
    stage_ref, stage_hidden_ref, send_sem, recv_sem, in_sem, out_sem = refs
    me_tp, me_ep = lax.axis_index('tp'), lax.axis_index('ep')
    right, left, across = lax.rem(me_tp + 1, tp), lax.rem(me_tp + tp - 1, tp), lax.rem(me_tp + 2, tp)
    east, west, beyond = lax.rem(me_ep + 2, ep), lax.rem(me_ep + ep - 2, ep), lax.rem(me_ep + 4, ep)
    partner = me_ep + 1 - 2 * lax.rem(me_ep, 2)
    peers = ({'tp': right}, {'tp': left}, {'tp': across}, {'ep': east}, {'ep': west}, {'ep': partner})
    to_right, to_left, to_across, to_east, to_west, to_partner = peers

    barrier = pltpu.get_barrier_semaphore()
    for peer in peers:
        pl.semaphore_signal(barrier, inc=1, device_id=peer, device_id_type=MESH)
    pl.semaphore_wait(barrier, len(peers))

    copies = []

    def send(source, target, peer):
        index = len(copies)
        copy = pltpu.make_async_remote_copy(src_ref=source, dst_ref=target, send_sem=send_sem.at[index], recv_sem=recv_sem.at[index],
                                            device_id=peer, device_id_type=MESH)
        copy.start()
        copies.append(copy)
        return copy

    rows = sources[0].shape[1]
    halves = (slice(0, rows // 2), slice(rows // 2, rows))
    sliced = [block for block in range(num_blocks) if block != direct]
    locals_in = [pltpu.make_async_copy(sources[block], stage_ref.at[block], in_sem.at[block]) for block in range(num_blocks)]
    locals_in.append(pltpu.make_async_copy(hidden_ref.at[me_tp], stage_hidden_ref, in_sem.at[num_blocks]))

    first = {}
    for block in sliced:
        first[block] = [send(sources[block].at[me_ep], gathered[block].at[me_tp, me_ep], peer) for peer in (to_right, to_left)]
    tables = [send(table_ref, tables_ref.at[me_tp], peer) for peer in (to_right, to_left, to_across)]
    for copy in locals_in:
        copy.start()
    tables_ref[me_tp] = table_ref[...]
    part = hidden_ref.shape[1] // 2
    relays = [send(hidden_ref.at[across, 0:part], relay_ref.at[0], to_right), send(hidden_ref.at[across, part:2 * part], relay_ref.at[1], to_left)]

    def share(block, group, index, span=None):
        ref = gathered[block]
        return ref.at[group, index] if span is None else ref.at[group, index, span]

    received = []
    forward, sideways = {}, {}
    for block in sliced:
        first[block][0].wait_recv()
        forward[block] = [send(share(block, left, me_ep, halves[0]), share(block, left, me_ep, halves[0]), to_right)]
        sideways[block] = {}
        for group, name in ((left, 'left'), (right, 'right')):
            if name == 'right':
                first[block][1].wait_recv()
                forward[block].append(send(share(block, right, me_ep, halves[1]), share(block, right, me_ep, halves[1]), to_left))
            whole = share(block, group, me_ep)
            sideways[block][name] = [send(whole, whole, to_east), send(whole, whole, to_west)]
            received.append(send(whole, whole, to_partner))
    core_half = ep // 2
    base = lax.rem(me_ep, 2) * core_half
    near = pl.ds(base, core_half)
    direct_first = [send(sources[direct].at[near], gathered[direct].at[me_tp, near], peer) for peer in (to_right, to_left)]
    swaps = [send(hidden_ref.at[right], seqs_ref.at[:, me_tp], to_right), send(hidden_ref.at[left], seqs_ref.at[:, me_tp], to_left)]
    for block in sliced:
        for copy in forward[block]:
            copy.wait_recv()
        whole = share(block, across, me_ep)
        sideways[block]['across'] = [send(whole, whole, to_east), send(whole, whole, to_west)]
        received.append(send(whole, whole, to_partner))
    for copy in relays:
        copy.wait_recv()
    swaps.append(send(relay_ref.at[0], seqs_ref.at[0:part, left], to_right))
    swaps.append(send(relay_ref.at[1], seqs_ref.at[part:2 * part, right], to_left))
    for copy in locals_in:
        copy.wait()
    locals_out = [pltpu.make_async_copy(stage_ref.at[block], gathered[block].at[me_tp], out_sem.at[block]) for block in range(num_blocks)]
    locals_out.append(pltpu.make_async_copy(stage_hidden_ref, seqs_ref.at[:, me_tp], out_sem.at[num_blocks]))
    for copy in locals_out:
        copy.start()

    def direct_ring():
        for copy in direct_first:
            copy.wait_recv()
        lower, upper = pl.ds(base, core_half // 2), pl.ds(base + core_half // 2, core_half // 2)
        last = [send(gathered[direct].at[left, lower], gathered[direct].at[left, lower], to_right),
                send(gathered[direct].at[right, upper], gathered[direct].at[right, upper], to_left)]
        for group in (left, right):
            received.append(send(gathered[direct].at[group, near], gathered[direct].at[group, near], to_partner))
        return last

    direct_last = None
    final = []
    groups = {'left': left, 'right': right, 'across': across}
    for count, block in enumerate(sliced):
        for name in ('left', 'right', 'across'):
            group = groups[name]
            sideways[block][name][0].wait_recv()
            pair = [send(share(block, group, west, halves[0]), share(block, group, west, halves[0]), to_east)]
            whole = share(block, group, west)
            received.append(send(whole, whole, to_partner))
            sideways[block][name][1].wait_recv()
            pair.append(send(share(block, group, east, halves[1]), share(block, group, east, halves[1]), to_west))
            whole = share(block, group, east)
            received.append(send(whole, whole, to_partner))
            final.append((block, group, pair))
        if count == 1:
            direct_last = direct_ring()
    for block, group, pair in final:
        for copy in pair:
            copy.wait_recv()
        whole = share(block, group, beyond)
        received.append(send(whole, whole, to_partner))
    for copy in direct_last:
        copy.wait_recv()
    whole = gathered[direct].at[across, near]
    received.append(send(whole, whole, to_partner))
    for copy in tables + swaps + received:
        copy.wait_recv()
    for copy in copies:
        copy.wait_send()
    for copy in locals_out:
        copy.wait()


def gather_all(hidden_in, table, blocks, direct, tp, ep):
    num_blocks = len(blocks)
    batch, local_seq, d_model = hidden_in.shape
    seqs = batch // tp
    hidden_view = hidden_in.reshape(tp, seqs, local_seq, d_model)
    views = [block.reshape(ep, block.shape[0] // ep, block.shape[1]) for block in blocks]
    any_spec = pl.BlockSpec(memory_space=pl.ANY)
    vmem_spec = pl.BlockSpec(memory_space=pltpu.VMEM)
    copies = 28 * (num_blocks - 1) + 7 + 9
    results = pl.pallas_call(
        functools.partial(gather_kernel, tp, ep, num_blocks, direct),
        in_specs=[any_spec, vmem_spec] + [any_spec] * num_blocks,
        out_specs=[any_spec, any_spec, vmem_spec] + [any_spec] * num_blocks,
        out_shape=[jax.ShapeDtypeStruct((seqs, tp, local_seq, d_model), hidden_in.dtype),
                   jax.ShapeDtypeStruct((2, seqs // 2, local_seq, d_model), hidden_in.dtype),
                   jax.ShapeDtypeStruct((tp,) + table.shape, table.dtype)]
        + [jax.ShapeDtypeStruct((tp,) + view.shape, view.dtype) for view in views],
        scratch_shapes=[pltpu.VMEM((num_blocks,) + views[0].shape, views[0].dtype), pltpu.VMEM((seqs, local_seq, d_model), hidden_in.dtype),
                        pltpu.SemaphoreType.DMA((copies,)), pltpu.SemaphoreType.DMA((copies,)),
                        pltpu.SemaphoreType.DMA((num_blocks + 1,)), pltpu.SemaphoreType.DMA((num_blocks + 1,))],
        compiler_params=pltpu.CompilerParams(collective_id=0, has_side_effects=True),
        name='gather_all',
    )(hidden_view, table, *views)
    hidden = results[0].reshape(seqs, tp * local_seq, d_model)
    tables = jnp.swapaxes(results[2], 0, 1).reshape(table.shape[0], -1, table.shape[2])
    return hidden, tables, [block.reshape(tp, -1, d_model) for block in results[3:]]


def attention_kernel(tp, hidden_ref, ln_ref, w_ref, table_ref, out_ref, keys_ref, values_ref, bias_ref, q_ref, kt_ref, ctx_ref, w_out_ref):
    seq_len, d_model = hidden_ref.shape[1], hidden_ref.shape[2]
    num_heads = table_ref.shape[0]
    head_dim = d_model // num_heads
    half = seq_len // 2
    width = d_model // tp
    starts = tuple(range(EXACT_BUCKETS + 1)) + THRESHOLDS

    @pl.when(pl.program_id(0) == 0)
    def _():
        def one_head(head, carry):
            for block in range(2):
                key_pos = lax.broadcasted_iota(jnp.int32, (half, half), 0)
                query_pos = lax.broadcasted_iota(jnp.int32, (half, half), 1) + block * half
                rel_pos = query_pos - key_pos
                bias = jnp.full((half, half), -jnp.inf, jnp.float32)
                for bucket, start in enumerate(starts):
                    bias = jnp.where(rel_pos >= start, table_ref[head, bucket], bias)
                bias_ref[head, :, block * half:(block + 1) * half] = bias
            return carry

        lax.fori_loop(0, num_heads, one_head, 0)
        for part in range(tp):
            w_out_ref[part * width:(part + 1) * width] = w_ref[part, 3 * width:]

    rows = hidden_ref[0].astype(jnp.float32)
    inv_rms = lax.rsqrt(jnp.mean(rows * rows, axis=-1, keepdims=True) + EPSILON)
    normed = (rows * inv_rms * ln_ref[...]).astype(jnp.bfloat16)
    nt = (((1,), (1,)), ((), ()))
    for part in range(tp):
        take = slice(part * width, (part + 1) * width)
        qkv = lax.dot_general(w_ref[part, :3 * width], normed, nt, preferred_element_type=jnp.float32).astype(jnp.bfloat16)
        q_ref[take] = qkv[:width]
        keys_ref[part, 0] = qkv[width:2 * width]
        values_ref[part, 0] = qkv[2 * width:]
        kt_ref[take] = qkv[width:2 * width]

    local_heads = num_heads // tp
    zeros = jnp.zeros((head_dim, seq_len), jnp.bfloat16)
    for head in range(num_heads):
        pair = slice((head // 2) * 2 * head_dim, (head // 2 + 1) * 2 * head_dim)
        q_head = q_ref[head * head_dim:(head + 1) * head_dim]
        q_pair = jnp.concatenate([q_head, zeros] if head % 2 == 0 else [zeros, q_head], axis=0)
        scores = jnp.dot(kt_ref[pair].T, q_pair, preferred_element_type=jnp.float32)
        value = values_ref[head // local_heads, 0, (head % local_heads) * head_dim:(head % local_heads + 1) * head_dim]
        near, far = bias_ref[head, :, :half], bias_ref[head, :, half:]
        scale = head_dim ** -0.5
        first = scores[:half, :half] * scale + near
        first = jnp.exp(first - jnp.max(first, axis=0, keepdims=True))
        probs = (first / jnp.sum(first, axis=0, keepdims=True)).astype(jnp.bfloat16)
        ctx_first = jnp.dot(value[:, :half], probs, preferred_element_type=jnp.float32)
        low = scores[:half, half:] * scale + far
        high = scores[half:, half:] * scale + near
        top = jnp.maximum(jnp.max(low, axis=0, keepdims=True), jnp.max(high, axis=0, keepdims=True))
        low, high = jnp.exp(low - top), jnp.exp(high - top)
        total = jnp.sum(low, axis=0, keepdims=True) + jnp.sum(high, axis=0, keepdims=True)
        probs = jnp.concatenate([(low / total).astype(jnp.bfloat16), (high / total).astype(jnp.bfloat16)], axis=0)
        ctx_second = jnp.dot(value, probs, preferred_element_type=jnp.float32)
        ctx = jnp.concatenate([ctx_first, ctx_second], axis=1)
        ctx_ref[head * head_dim:(head + 1) * head_dim] = ctx.astype(jnp.bfloat16)
    attn_out = jnp.dot(ctx_ref[...].T, w_out_ref[...], preferred_element_type=jnp.float32)
    out_ref[0] = (rows + attn_out).astype(jnp.bfloat16)


def attention(hidden, ln_scale, packed, table, tp):
    seqs, seq_len, d_model = hidden.shape
    num_heads = table.shape[0]
    width = d_model // tp
    seq_block = pl.BlockSpec((1, seq_len, d_model), lambda s: (s, 0, 0))
    cache_block = pl.BlockSpec((tp, 1, width, seq_len), lambda s: (0, s, 0, 0))
    cache = jax.ShapeDtypeStruct((tp, seqs, width, seq_len), jnp.bfloat16)
    flops = 2 * seqs * seq_len * d_model * (5 * d_model + 3 * seq_len)
    return pl.pallas_call(
        functools.partial(attention_kernel, tp),
        grid=(seqs,),
        in_specs=[seq_block, pl.BlockSpec((1, d_model), lambda s: (0, 0)), pl.BlockSpec((tp, d_model, d_model), lambda s: (0, 0, 0)),
                  pl.BlockSpec(memory_space=pltpu.SMEM)],
        out_specs=[seq_block, cache_block, cache_block],
        out_shape=[jax.ShapeDtypeStruct(hidden.shape, hidden.dtype), cache, cache],
        scratch_shapes=[pltpu.VMEM((num_heads, seq_len // 2, seq_len), jnp.float32), pltpu.VMEM((d_model, seq_len), jnp.bfloat16),
                        pltpu.VMEM((d_model, seq_len), jnp.bfloat16), pltpu.VMEM((d_model, seq_len), jnp.bfloat16),
                        pltpu.VMEM((d_model, d_model), jnp.bfloat16)],
        compiler_params=pltpu.CompilerParams(dimension_semantics=('arbitrary',), vmem_limit_bytes=40 * 1024 * 1024),
        cost_estimate=pl.CostEstimate(flops=flops, bytes_accessed=2 * (hidden.size * 4 + packed.size), transcendentals=0),
        name='attention',
    )(hidden, ln_scale[None], packed, table)


def dense_ffn(hidden, ln_scale, gate, up, down):
    normed = rms_norm(hidden, ln_scale)
    gate_pre = jnp.einsum('std,gdf->stgf', normed, gate, preferred_element_type=jnp.float32)
    up_pre = jnp.einsum('std,gdf->stgf', normed, up, preferred_element_type=jnp.float32)
    ffn_hidden = (jax.nn.gelu(gate_pre) * up_pre).astype(jnp.bfloat16)
    ffn_out = jnp.einsum('stgf,gfd->std', ffn_hidden, down, preferred_element_type=jnp.float32)
    return (hidden.astype(jnp.float32) + ffn_out).astype(jnp.bfloat16)


def moe_kernel(tp, ep, ff_tile, sent_ref, w_in_ref, w_out_ref, keys_ref, values_ref, back_ref, keys_out_ref, values_out_ref, turn_ref, relay_kv_ref, stage_ref, rows_ref, result_ref, relay_y_ref, relay_x_ref,
               in_slots, out_slots, send_sem, recv_sem, weight_sem, local_sem):
    me_tp, me_ep = lax.axis_index('tp'), lax.axis_index('ep')
    right, left, across = lax.rem(me_tp + 1, tp), lax.rem(me_tp + tp - 1, tp), lax.rem(me_tp + 2, tp)

    def partner_of(index):
        return index + 1 - 2 * lax.rem(index, 2)

    partner = partner_of(me_ep)
    east, west, beyond = lax.rem(me_ep + 2, ep), lax.rem(me_ep + ep - 2, ep), lax.rem(me_ep + 4, ep)
    east_other, west_other, beyond_other = partner_of(east), partner_of(west), partner_of(beyond)
    peers = [{'tp': right}, {'tp': left}] + [{'ep': index} for index in (partner, east, east_other, west, west_other)]
    to_right, to_left = peers[:2]

    barrier = pltpu.get_barrier_semaphore()
    for peer in peers:
        pl.semaphore_signal(barrier, inc=1, device_id=peer, device_id_type=MESH)
    pl.semaphore_wait(barrier, len(peers))

    experts = w_in_ref.shape[0]
    half_y, half_x = ep // 2, tp // 2
    copies, local_copies = [], []

    def send(source, target, peer):
        index = len(copies)
        copy = pltpu.make_async_remote_copy(src_ref=source, dst_ref=target, send_sem=send_sem.at[index], recv_sem=recv_sem.at[index],
                                            device_id=peer, device_id_type=MESH)
        copy.start()
        copies.append(copy)
        return copy

    def keep(source, target):
        copy = pltpu.make_async_copy(source, target, local_sem.at[len(local_copies)])
        copy.start()
        local_copies.append(copy)
        return copy

    def fetch(expert):
        slot = expert % 2
        pair = (pltpu.make_async_copy(w_in_ref.at[expert], in_slots.at[slot], weight_sem.at[slot, 0]),
                pltpu.make_async_copy(w_out_ref.at[expert], out_slots.at[slot], weight_sem.at[slot, 1]))
        for copy in pair:
            copy.start()
        return pair

    class Exchange:
        def __init__(self, way, expert, source, middle, target):
            self.source, self.middle, self.target = source, middle, target
            self.relay_y, self.relay_x = relay_y_ref.at[way, expert], relay_x_ref.at[way, expert]

        def start_y(self):
            self.hops = [send(self.source(across).at[0:half_y], self.relay_y.at[0], to_right),
                         send(self.source(across).at[half_y:ep], self.relay_y.at[1], to_left)]
            self.direct = [send(self.source(right), self.middle.at[me_tp], to_right), send(self.source(left), self.middle.at[me_tp], to_left)]
            self.own = keep(self.source(me_tp), self.middle.at[me_tp])

        def forward_y(self):
            self.hops[0].wait_recv()
            self.direct.append(send(self.relay_y.at[0], self.middle.at[left, 0:half_y], to_right))
            self.hops[1].wait_recv()
            self.direct.append(send(self.relay_y.at[1], self.middle.at[right, half_y:ep], to_left))

        def finish_y(self):
            for copy in self.direct:
                copy.wait_recv()
            self.own.wait()

        def start_x(self):
            self.hops, self.direct = [], []
            for way, (near, low, high) in enumerate(((east, 0, half_x), (west, half_x, tp))):
                for index, far in enumerate((beyond, beyond_other)):
                    self.hops.append(send(self.middle.at[low:high, far], self.relay_x.at[way, index], {'ep': near}))
            for near in (east, west, east_other, west_other, partner):
                self.direct.append(send(self.middle.at[:, near], self.target(me_ep), {'ep': near}))

        def forward_x(self):
            for way, (origin, low, high, ends) in enumerate(((west, 0, half_x, (east, east_other)), (east, half_x, tp, (west, west_other)))):
                for index, end in enumerate(ends):
                    self.hops[2 * way + index].wait_recv()
                    self.direct.append(send(self.relay_x.at[way, index], self.target(origin).at[low:high], {'ep': end}))

        def finish_x(self):
            for copy in self.direct:
                copy.wait_recv()

    def outward(expert):
        return Exchange(0, expert, lambda index: sent_ref.at[index, :, expert], stage_ref.at[expert],
                        lambda index: rows_ref.at[expert, :, index])

    def inward(expert):
        return Exchange(1, expert, lambda index: result_ref.at[expert, index], turn_ref.at[expert],
                        lambda index: back_ref.at[:, index, expert])

    def compute(expert, begin, end):
        slot = expert % 2
        if begin == 0:
            for copy in weights[expert]:
                copy.wait()
            rows_ref[expert, :, me_ep] = stage_ref[expert, :, me_ep]
        row_shape = rows_ref.shape[2:]
        d_model, ff_dim = w_in_ref.shape[1:]

        def one_tile(tile, carry):
            rows = rows_ref[expert, tile].reshape(row_shape[0] * row_shape[1], row_shape[2])
            total = None
            for start in range(0, ff_dim, ff_tile):
                pre = jnp.dot(rows, in_slots[slot, :, start:start + ff_tile], preferred_element_type=jnp.float32)
                act = jax.nn.gelu(pre).astype(jnp.bfloat16)
                part = jnp.dot(act, out_slots[slot, start:start + ff_tile], preferred_element_type=jnp.float32)
                total = part if total is None else total + part
            result_ref[expert, tile] = total.astype(jnp.bfloat16).reshape(row_shape)
            return carry

        lax.fori_loop(begin, end, one_tile, 0)

    out = [outward(expert) for expert in range(experts)]
    ret = [inward(expert) for expert in range(experts)]
    chain = out + ret
    weights = {}
    last = len(chain) - 1
    chain[0].start_y()
    weights[0] = fetch(0)
    weights[1] = fetch(1)
    for step in range(last + 2):
        expert = step - 2
        if 0 <= expert < experts:
            compute(expert, 0, 1)
        if step <= last:
            chain[step].forward_y()
            if step < last:
                chain[step + 1].start_y()
        if step >= 1:
            chain[step - 1].forward_x()
        if 0 <= expert < experts:
            compute(expert, 1, tp)
            if expert + 2 < experts:
                weights[expert + 2] = fetch(expert + 2)
        if step <= last:
            chain[step].finish_y()
            chain[step].start_x()
        if 1 <= step <= experts:
            out[step - 1].finish_x()
        if step == last - 1:
            near_seqs = keys_ref.shape[1] // 2
            spans = (slice(0, near_seqs), slice(near_seqs, 2 * near_seqs))
            pairs = ((keys_ref, keys_out_ref), (values_ref, values_out_ref))
            cache_own = [keep(source.at[me_tp], target.at[me_tp]) for source, target in pairs]
        if step == last:
            cache_hops = [send(source.at[across, spans[way]], relay_kv_ref.at[index, way], peer)
                          for index, (source, _) in enumerate(pairs) for way, peer in enumerate((to_right, to_left))]
            cache_moves = [send(source.at[goal], target.at[me_tp], peer)
                           for source, target in pairs for goal, peer in ((right, to_right), (left, to_left))]
    own = [keep(turn_ref.at[expert, :, me_ep], back_ref.at[:, me_ep, expert]) for expert in range(experts)]
    for index, (_, target) in enumerate(pairs):
        for way, (origin, peer) in enumerate(((left, to_right), (right, to_left))):
            cache_hops[2 * index + way].wait_recv()
            cache_moves.append(send(relay_kv_ref.at[index, way], target.at[origin, spans[way]], peer))
    for exchange in ret:
        exchange.finish_x()
    for copy in cache_moves:
        copy.wait_recv()
    for copy in cache_own:
        copy.wait()
    for copy in own:
        copy.wait()
    for copy in copies:
        copy.wait_send()


def moe_exchange(dispatched, expert_in, expert_out, keys, values, tp, ep):
    experts, d_model, ff_dim = expert_in.shape
    slots = dispatched.shape[0] // (tp * ep * experts)
    view = dispatched.reshape(tp, ep, experts, slots, d_model)
    any_spec = pl.BlockSpec(memory_space=pl.ANY)
    rows = (experts, tp, ep, slots, d_model)
    count = experts * 2 * (6 + 13) + 12
    cache = jax.ShapeDtypeStruct(keys.shape, keys.dtype)
    relay = jax.ShapeDtypeStruct((2, 2, keys.shape[1] // 2) + keys.shape[2:], keys.dtype)
    dtype = dispatched.dtype
    total_rows = dispatched.shape[0]
    back, keys, values, _, _ = pl.pallas_call(
        functools.partial(moe_kernel, tp, ep, ff_dim // 4),
        in_specs=[any_spec] * 5,
        out_specs=[any_spec] * 5,
        out_shape=[jax.ShapeDtypeStruct(view.shape, dtype), cache, cache, jax.ShapeDtypeStruct(rows, dtype), relay],
        scratch_shapes=[pltpu.VMEM(rows, dtype), pltpu.VMEM(rows, dtype), pltpu.VMEM(rows, dtype),
                        pltpu.VMEM((2, experts, 2, ep // 2, slots, d_model), dtype), pltpu.VMEM((2, experts, 2, 2, tp // 2, slots, d_model), dtype),
                        pltpu.VMEM((2, d_model, ff_dim), dtype), pltpu.VMEM((2, ff_dim, d_model), dtype),
                        pltpu.SemaphoreType.DMA((count,)), pltpu.SemaphoreType.DMA((count,)), pltpu.SemaphoreType.DMA((2, 2)),
                        pltpu.SemaphoreType.DMA((3 * experts + 2,))],
        compiler_params=pltpu.CompilerParams(collective_id=1, has_side_effects=True, vmem_limit_bytes=62 * 1024 * 1024),
        cost_estimate=pl.CostEstimate(flops=4 * total_rows * d_model * ff_dim, bytes_accessed=4 * expert_in.size, transcendentals=0),
        name='moe_exchange',
    )(view, expert_in, expert_out, keys, values)
    return back.reshape(dispatched.shape), keys, values


def slot_table(choices, num_experts):
    experts = jnp.arange(num_experts, dtype=jnp.int32)
    first_hot = (choices[..., 0:1] == experts).astype(jnp.int32)
    second_hot = (choices[..., 1:2] == experts).astype(jnp.int32)
    first_pos = jnp.sum((jnp.cumsum(first_hot, axis=-2) - 1) * first_hot, axis=-1)
    second_base = jnp.cumsum(second_hot, axis=-2) - 1 + jnp.sum(first_hot, axis=-2, keepdims=True)
    second_pos = jnp.sum(second_base * second_hot, axis=-1)
    return jnp.stack([first_pos, second_pos], axis=-1)


def moe_block(hidden, ln_scale, w_router, expert_in, expert_out, expert_ids, caches, tp, ep):
    local_batch, local_seq, d_model = hidden.shape
    tokens = local_batch * local_seq
    num_experts = w_router.shape[1]
    capacity = 4 * tokens // num_experts
    choices = expert_ids.reshape(tokens, 2)
    position = slot_table(choices, num_experts)
    slot_ids = jnp.where(position < capacity, choices * capacity + position, -1)
    columns = jnp.arange(num_experts * capacity, dtype=jnp.int32)
    select = (slot_ids[:, :, None] == columns).astype(jnp.bfloat16)

    normed = rms_norm(hidden, ln_scale).reshape(tokens, d_model)
    dispatched = jnp.einsum('ncs,nd->sd', select, normed, preferred_element_type=jnp.float32).astype(jnp.bfloat16)
    returned, *caches = moe_exchange(dispatched, expert_in, expert_out, *caches, tp, ep)

    logits = jnp.dot(normed.astype(jnp.float32), w_router, precision=lax.Precision.HIGHEST)
    router_probs = jax.nn.softmax(logits, axis=-1)
    experts = jnp.arange(num_experts, dtype=jnp.int32)
    picked = jnp.sum(jnp.where(choices[:, :, None] == experts, router_probs[:, None, :], 0.0), axis=-1)
    gate_weights = picked / jnp.sum(picked, axis=-1, keepdims=True)

    gathered_out = jnp.einsum('ncs,sd->ncd', select, returned, preferred_element_type=jnp.float32)
    moe_sum = jnp.sum(gate_weights[:, :, None] * gathered_out, axis=1).reshape(local_batch, local_seq, d_model)
    return (hidden.astype(jnp.float32) + moe_sum).astype(jnp.bfloat16), *caches


def solution(mesh):
    tp, ep = mesh.shape['tp'], mesh.shape['ep']
    act_spec = P(('dp', 'ep'), 'tp', None)
    col_spec = P(None, None, 'tp')
    row_spec = P(None, 'tp', None)
    expert_spec = P(('tp', 'ep'), None, None)
    cache_spec = P(None, ('dp', 'ep'), 'tp', None, None)
    in_specs = (act_spec, P(), P(), col_spec, col_spec, col_spec, row_spec, row_spec,
                P(None, 'tp'), P(None, 'tp'), P('tp', None), P(), expert_spec, expert_spec, act_spec)

    def as_cache(got, local_heads):
        return jnp.swapaxes(got.reshape(got.shape[0] * got.shape[1], local_heads, -1, got.shape[3]), 2, 3)

    def device_fn(hidden_in, ln_attn, ln_ffn, w_query, w_key, w_value, w_out, bias_table, w_gate, w_up, w_down, w_router, expert_in, expert_out, expert_ids):
        def packed(layer):
            parts = [jnp.swapaxes(w[layer], 0, 1) for w in (w_query, w_key, w_value)] + [w_out[layer]]
            return jnp.concatenate(parts, axis=0)

        local_heads = bias_table.shape[1]
        blocks = [packed(0), w_up, w_down, packed(1), w_gate]
        hidden, tables, (attn_zero, up, down, attn_one, gate) = gather_all(hidden_in, bias_table, blocks, len(blocks) - 1, tp, ep)
        hidden, keys_zero, values_zero = attention(hidden, ln_attn[0], attn_zero, tables[0], tp)
        keys_zero, values_zero = tp_exchange_permutes(keys_zero, tp), tp_exchange_permutes(values_zero, tp)
        hidden = dense_ffn(hidden, ln_ffn[0], gate, up, down)
        hidden, keys_one, values_one = attention(hidden, ln_attn[1], attn_one, tables[1], tp)
        hidden, keys_zero, values_zero = lax.optimization_barrier((hidden, keys_zero, values_zero))
        hidden = lax.all_to_all(hidden, 'tp', 1, 0, tiled=True)
        hidden, keys_one, values_one = moe_block(hidden, ln_ffn[1], w_router, expert_in, expert_out, expert_ids, (keys_one, values_one), tp, ep)
        keys = jnp.stack([as_cache(keys_zero, local_heads), as_cache(keys_one, local_heads)])
        values = jnp.stack([as_cache(values_zero, local_heads), as_cache(values_one, local_heads)])
        return hidden, keys, values

    return jax.shard_map(device_fn, mesh=mesh, in_specs=in_specs, out_specs=(act_spec, cache_spec, cache_spec), check_vma=False)
```

```python
import functools

import jax
import jax.numpy as jnp
from jax import lax
from jax.experimental import pallas as pl
from jax.experimental.pallas import tpu as pltpu
from jax.sharding import PartitionSpec as P

EXACT_BUCKETS = 16
THRESHOLDS = (18, 20, 23, 26, 30, 34, 39, 45, 51, 58, 66, 76, 86, 98, 112)
EPSILON = 1e-6
GROUP = ('tp', 'ep')
MESH = pl.DeviceIdType.MESH


def rms_norm(rows_in, ln_scale):
    wide_rows = rows_in.astype(jnp.float32)
    inv_rms = lax.rsqrt(jnp.mean(wide_rows * wide_rows, axis=-1, keepdims=True) + EPSILON)
    return (wide_rows * inv_rms * ln_scale).astype(jnp.bfloat16)


def gather_kernel(tp, ep, num_blocks, direct, hidden_ref, table_ref, *refs):
    sources, refs = refs[:num_blocks], refs[num_blocks:]
    seqs_ref, relay_ref, tables_ref, refs = refs[0], refs[1], refs[2], refs[3:]
    gathered, refs = refs[:num_blocks], refs[num_blocks:]
    stage_ref, stage_hidden_ref, send_sem, recv_sem, in_sem, out_sem = refs
    me_tp, me_ep = lax.axis_index('tp'), lax.axis_index('ep')
    right, left, across = lax.rem(me_tp + 1, tp), lax.rem(me_tp + tp - 1, tp), lax.rem(me_tp + 2, tp)
    east, west, beyond = lax.rem(me_ep + 2, ep), lax.rem(me_ep + ep - 2, ep), lax.rem(me_ep + 4, ep)
    partner = me_ep + 1 - 2 * lax.rem(me_ep, 2)
    peers = ({'tp': right}, {'tp': left}, {'tp': across}, {'ep': east}, {'ep': west}, {'ep': partner})
    to_right, to_left, to_across, to_east, to_west, to_partner = peers

    barrier = pltpu.get_barrier_semaphore()
    for peer in peers:
        pl.semaphore_signal(barrier, inc=1, device_id=peer, device_id_type=MESH)
    pl.semaphore_wait(barrier, len(peers))

    copies = []

    def send(source, target, peer):
        index = len(copies)
        copy = pltpu.make_async_remote_copy(src_ref=source, dst_ref=target, send_sem=send_sem.at[index], recv_sem=recv_sem.at[index],
                                            device_id=peer, device_id_type=MESH)
        copy.start()
        copies.append(copy)
        return copy

    rows = sources[0].shape[1]
    halves = (slice(0, rows // 2), slice(rows // 2, rows))
    sliced = [block for block in range(num_blocks) if block != direct]
    locals_in = [pltpu.make_async_copy(sources[block], stage_ref.at[block], in_sem.at[block]) for block in range(num_blocks)]
    locals_in.append(pltpu.make_async_copy(hidden_ref.at[me_tp], stage_hidden_ref, in_sem.at[num_blocks]))

    first = {}
    for block in sliced:
        first[block] = [send(sources[block].at[me_ep], gathered[block].at[me_tp, me_ep], peer) for peer in (to_right, to_left)]
    tables = [send(table_ref, tables_ref.at[me_tp], peer) for peer in (to_right, to_left, to_across)]
    for copy in locals_in:
        copy.start()
    tables_ref[me_tp] = table_ref[...]
    part = hidden_ref.shape[1] // 2
    relays = [send(hidden_ref.at[across, 0:part], relay_ref.at[0], to_right), send(hidden_ref.at[across, part:2 * part], relay_ref.at[1], to_left)]

    def share(block, group, index, span=None):
        ref = gathered[block]
        return ref.at[group, index] if span is None else ref.at[group, index, span]

    received = []
    forward, sideways = {}, {}
    for block in sliced:
        first[block][0].wait_recv()
        forward[block] = [send(share(block, left, me_ep, halves[0]), share(block, left, me_ep, halves[0]), to_right)]
        sideways[block] = {}
        for group, name in ((left, 'left'), (right, 'right')):
            if name == 'right':
                first[block][1].wait_recv()
                forward[block].append(send(share(block, right, me_ep, halves[1]), share(block, right, me_ep, halves[1]), to_left))
            whole = share(block, group, me_ep)
            sideways[block][name] = [send(whole, whole, to_east), send(whole, whole, to_west)]
            received.append(send(whole, whole, to_partner))
    core_half = ep // 2
    base = lax.rem(me_ep, 2) * core_half
    near = pl.ds(base, core_half)
    direct_first = [send(sources[direct].at[near], gathered[direct].at[me_tp, near], peer) for peer in (to_right, to_left)]
    swaps = [send(hidden_ref.at[right], seqs_ref.at[:, me_tp], to_right), send(hidden_ref.at[left], seqs_ref.at[:, me_tp], to_left)]
    for block in sliced:
        for copy in forward[block]:
            copy.wait_recv()
        whole = share(block, across, me_ep)
        sideways[block]['across'] = [send(whole, whole, to_east), send(whole, whole, to_west)]
        received.append(send(whole, whole, to_partner))
    for copy in relays:
        copy.wait_recv()
    swaps.append(send(relay_ref.at[0], seqs_ref.at[0:part, left], to_right))
    swaps.append(send(relay_ref.at[1], seqs_ref.at[part:2 * part, right], to_left))
    for copy in locals_in:
        copy.wait()
    locals_out = [pltpu.make_async_copy(stage_ref.at[block], gathered[block].at[me_tp], out_sem.at[block]) for block in range(num_blocks)]
    locals_out.append(pltpu.make_async_copy(stage_hidden_ref, seqs_ref.at[:, me_tp], out_sem.at[num_blocks]))
    for copy in locals_out:
        copy.start()

    def direct_ring():
        for copy in direct_first:
            copy.wait_recv()
        lower, upper = pl.ds(base, core_half // 2), pl.ds(base + core_half // 2, core_half // 2)
        last = [send(gathered[direct].at[left, lower], gathered[direct].at[left, lower], to_right),
                send(gathered[direct].at[right, upper], gathered[direct].at[right, upper], to_left)]
        for group in (left, right):
            received.append(send(gathered[direct].at[group, near], gathered[direct].at[group, near], to_partner))
        return last

    direct_last = None
    final = []
    groups = {'left': left, 'right': right, 'across': across}
    for count, block in enumerate(sliced):
        for name in ('left', 'right', 'across'):
            group = groups[name]
            sideways[block][name][0].wait_recv()
            pair = [send(share(block, group, west, halves[0]), share(block, group, west, halves[0]), to_east)]
            whole = share(block, group, west)
            received.append(send(whole, whole, to_partner))
            sideways[block][name][1].wait_recv()
            pair.append(send(share(block, group, east, halves[1]), share(block, group, east, halves[1]), to_west))
            whole = share(block, group, east)
            received.append(send(whole, whole, to_partner))
            final.append((block, group, pair))
        if count == 1:
            direct_last = direct_ring()
    for block, group, pair in final:
        for copy in pair:
            copy.wait_recv()
        whole = share(block, group, beyond)
        received.append(send(whole, whole, to_partner))
    for copy in direct_last:
        copy.wait_recv()
    whole = gathered[direct].at[across, near]
    received.append(send(whole, whole, to_partner))
    for copy in tables + swaps + received:
        copy.wait_recv()
    for copy in copies:
        copy.wait_send()
    for copy in locals_out:
        copy.wait()


def gather_all(hidden_in, table, blocks, direct, tp, ep):
    num_blocks = len(blocks)
    batch, local_seq, d_model = hidden_in.shape
    seqs = batch // tp
    hidden_view = hidden_in.reshape(tp, seqs, local_seq, d_model)
    views = [block.reshape(ep, block.shape[0] // ep, block.shape[1]) for block in blocks]
    any_spec = pl.BlockSpec(memory_space=pl.ANY)
    vmem_spec = pl.BlockSpec(memory_space=pltpu.VMEM)
    copies = 28 * (num_blocks - 1) + 7 + 9
    results = pl.pallas_call(
        functools.partial(gather_kernel, tp, ep, num_blocks, direct),
        in_specs=[any_spec, vmem_spec] + [any_spec] * num_blocks,
        out_specs=[any_spec, any_spec, vmem_spec] + [any_spec] * num_blocks,
        out_shape=[jax.ShapeDtypeStruct((seqs, tp, local_seq, d_model), hidden_in.dtype),
                   jax.ShapeDtypeStruct((2, seqs // 2, local_seq, d_model), hidden_in.dtype),
                   jax.ShapeDtypeStruct((tp,) + table.shape, table.dtype)]
        + [jax.ShapeDtypeStruct((tp,) + view.shape, view.dtype) for view in views],
        scratch_shapes=[pltpu.VMEM((num_blocks,) + views[0].shape, views[0].dtype), pltpu.VMEM((seqs, local_seq, d_model), hidden_in.dtype),
                        pltpu.SemaphoreType.DMA((copies,)), pltpu.SemaphoreType.DMA((copies,)),
                        pltpu.SemaphoreType.DMA((num_blocks + 1,)), pltpu.SemaphoreType.DMA((num_blocks + 1,))],
        compiler_params=pltpu.CompilerParams(collective_id=0, has_side_effects=True),
        name='gather_all',
    )(hidden_view, table, *views)
    hidden = results[0].reshape(seqs, tp * local_seq, d_model)
    tables = jnp.swapaxes(results[2], 0, 1).reshape(table.shape[0], -1, table.shape[2])
    return hidden, tables, [block.reshape(tp, -1, d_model) for block in results[3:]]


def attention_kernel(tp, moving, hidden_ref, ln_ref, w_ref, table_ref, *refs):
    if moving:
        old_keys_ref, old_values_ref, out_ref, keys_ref, values_ref, new_keys_ref, new_values_ref = refs[:7]
        relay_ref, send_sem, recv_sem, local_sem = refs[12:]
        bias_ref, q_ref, kt_ref, ctx_ref, w_out_ref = refs[7:12]
    else:
        out_ref, keys_ref, values_ref, bias_ref, q_ref, kt_ref, ctx_ref, w_out_ref = refs
    seq_len, d_model = hidden_ref.shape[1], hidden_ref.shape[2]
    num_heads = table_ref.shape[0]
    head_dim = d_model // num_heads
    half = seq_len // 2
    width = d_model // tp
    starts = tuple(range(EXACT_BUCKETS + 1)) + THRESHOLDS

    if moving:
        me_tp = lax.axis_index('tp')
        right, left, across = lax.rem(me_tp + 1, tp), lax.rem(me_tp + tp - 1, tp), lax.rem(me_tp + 2, tp)
        pairs = ((old_keys_ref, new_keys_ref), (old_values_ref, new_values_ref))
        half_seqs = old_keys_ref.shape[1] // 2
        spans = (slice(0, half_seqs), slice(half_seqs, 2 * half_seqs))

        def remote(index, source, target, to):
            return pltpu.make_async_remote_copy(src_ref=source, dst_ref=target, send_sem=send_sem.at[index], recv_sem=recv_sem.at[index],
                                                device_id={'tp': to}, device_id_type=MESH)

        hops, directs, forwards, owns = [], [], [], []
        for index, (source, target) in enumerate(pairs):
            for way, (goal, origin) in enumerate(((right, left), (left, right))):
                number = 2 * index + way
                hops.append(remote(number, source.at[across, spans[way]], relay_ref.at[index, way], goal))
                directs.append(remote(4 + number, source.at[goal], target.at[me_tp], goal))
                forwards.append(remote(8 + number, relay_ref.at[index, way], target.at[origin, spans[way]], goal))
            owns.append(pltpu.make_async_copy(source.at[me_tp], target.at[me_tp], local_sem.at[index]))

        @pl.when(pl.program_id(0) == 0)
        def _():
            barrier = pltpu.get_barrier_semaphore()
            for goal in (right, left):
                pl.semaphore_signal(barrier, inc=1, device_id={'tp': goal}, device_id_type=MESH)
            pl.semaphore_wait(barrier, 2)
            for copy in hops + directs + owns:
                copy.start()

        @pl.when(pl.program_id(0) == 2)
        def _():
            for hop, forward in zip(hops, forwards):
                hop.wait_recv()
                forward.start()

    @pl.when(pl.program_id(0) == 0)
    def _():
        def one_head(head, carry):
            for block in range(2):
                key_pos = lax.broadcasted_iota(jnp.int32, (half, half), 0)
                query_pos = lax.broadcasted_iota(jnp.int32, (half, half), 1) + block * half
                rel_pos = query_pos - key_pos
                bias = jnp.full((half, half), -jnp.inf, jnp.float32)
                for bucket, start in enumerate(starts):
                    bias = jnp.where(rel_pos >= start, table_ref[head, bucket], bias)
                bias_ref[head, :, block * half:(block + 1) * half] = bias
            return carry

        lax.fori_loop(0, num_heads, one_head, 0)
        for part in range(tp):
            w_out_ref[part * width:(part + 1) * width] = w_ref[part, 3 * width:]

    rows = hidden_ref[0].astype(jnp.float32)
    inv_rms = lax.rsqrt(jnp.mean(rows * rows, axis=-1, keepdims=True) + EPSILON)
    normed = (rows * inv_rms * ln_ref[...]).astype(jnp.bfloat16)
    nt = (((1,), (1,)), ((), ()))
    for part in range(tp):
        take = slice(part * width, (part + 1) * width)
        qkv = lax.dot_general(w_ref[part, :3 * width], normed, nt, preferred_element_type=jnp.float32).astype(jnp.bfloat16)
        q_ref[take] = qkv[:width]
        keys_ref[part, 0] = qkv[width:2 * width]
        values_ref[part, 0] = qkv[2 * width:]
        kt_ref[take] = qkv[width:2 * width]

    local_heads = num_heads // tp
    zeros = jnp.zeros((head_dim, seq_len), jnp.bfloat16)
    for head in range(num_heads):
        pair = slice((head // 2) * 2 * head_dim, (head // 2 + 1) * 2 * head_dim)
        q_head = q_ref[head * head_dim:(head + 1) * head_dim]
        q_pair = jnp.concatenate([q_head, zeros] if head % 2 == 0 else [zeros, q_head], axis=0)
        scores = jnp.dot(kt_ref[pair].T, q_pair, preferred_element_type=jnp.float32)
        value = values_ref[head // local_heads, 0, (head % local_heads) * head_dim:(head % local_heads + 1) * head_dim]
        near, far = bias_ref[head, :, :half], bias_ref[head, :, half:]
        scale = head_dim ** -0.5
        first = scores[:half, :half] * scale + near
        first = jnp.exp(first - jnp.max(first, axis=0, keepdims=True))
        probs = (first / jnp.sum(first, axis=0, keepdims=True)).astype(jnp.bfloat16)
        ctx_first = jnp.dot(value[:, :half], probs, preferred_element_type=jnp.float32)
        low = scores[:half, half:] * scale + far
        high = scores[half:, half:] * scale + near
        top = jnp.maximum(jnp.max(low, axis=0, keepdims=True), jnp.max(high, axis=0, keepdims=True))
        low, high = jnp.exp(low - top), jnp.exp(high - top)
        total = jnp.sum(low, axis=0, keepdims=True) + jnp.sum(high, axis=0, keepdims=True)
        probs = jnp.concatenate([(low / total).astype(jnp.bfloat16), (high / total).astype(jnp.bfloat16)], axis=0)
        ctx_second = jnp.dot(value, probs, preferred_element_type=jnp.float32)
        ctx = jnp.concatenate([ctx_first, ctx_second], axis=1)
        ctx_ref[head * head_dim:(head + 1) * head_dim] = ctx.astype(jnp.bfloat16)
    attn_out = jnp.dot(ctx_ref[...].T, w_out_ref[...], preferred_element_type=jnp.float32)
    out_ref[0] = (rows + attn_out).astype(jnp.bfloat16)

    if moving:
        @pl.when(pl.program_id(0) == pl.num_programs(0) - 1)
        def _():
            for copy in directs + forwards:
                copy.wait_recv()
            for copy in hops + directs + forwards:
                copy.wait_send()
            for copy in owns:
                copy.wait()


def attention(hidden, ln_scale, packed, table, tp, old=()):
    seqs, seq_len, d_model = hidden.shape
    num_heads = table.shape[0]
    width = d_model // tp
    seq_block = pl.BlockSpec((1, seq_len, d_model), lambda s: (s, 0, 0))
    cache_block = pl.BlockSpec((tp, 1, width, seq_len), lambda s: (0, s, 0, 0))
    cache = jax.ShapeDtypeStruct((tp, seqs, width, seq_len), jnp.bfloat16)
    flops = 2 * seqs * seq_len * d_model * (5 * d_model + 3 * seq_len)
    any_spec = pl.BlockSpec(memory_space=pl.ANY)
    scratch = [pltpu.VMEM((num_heads, seq_len // 2, seq_len), jnp.float32), pltpu.VMEM((d_model, seq_len), jnp.bfloat16),
               pltpu.VMEM((d_model, seq_len), jnp.bfloat16), pltpu.VMEM((d_model, seq_len), jnp.bfloat16),
               pltpu.VMEM((d_model, d_model), jnp.bfloat16)]
    options = {}
    if old:
        scratch += [pltpu.VMEM((2, 2, seqs // 2) + cache.shape[2:], jnp.bfloat16), pltpu.SemaphoreType.DMA((12,)),
                    pltpu.SemaphoreType.DMA((12,)), pltpu.SemaphoreType.DMA((2,))]
        options = dict(collective_id=2, has_side_effects=True)
    return pl.pallas_call(
        functools.partial(attention_kernel, tp, bool(old)),
        grid=(seqs,),
        in_specs=[seq_block, pl.BlockSpec((1, d_model), lambda s: (0, 0)), pl.BlockSpec((tp, d_model, d_model), lambda s: (0, 0, 0)),
                  pl.BlockSpec(memory_space=pltpu.SMEM)] + [any_spec] * len(old),
        out_specs=[seq_block, cache_block, cache_block] + [any_spec] * len(old),
        out_shape=[jax.ShapeDtypeStruct(hidden.shape, hidden.dtype), cache, cache] + [cache] * len(old),
        scratch_shapes=scratch,
        compiler_params=pltpu.CompilerParams(dimension_semantics=('arbitrary',), vmem_limit_bytes=40 * 1024 * 1024, **options),
        cost_estimate=pl.CostEstimate(flops=flops, bytes_accessed=2 * (hidden.size * 4 + packed.size), transcendentals=0),
        name='attention_moving' if old else 'attention',
    )(hidden, ln_scale[None], packed, table, *old)


def dense_ffn(hidden, ln_scale, gate, up, down):
    normed = rms_norm(hidden, ln_scale)
    gate_pre = jnp.einsum('std,gdf->stgf', normed, gate, preferred_element_type=jnp.float32)
    up_pre = jnp.einsum('std,gdf->stgf', normed, up, preferred_element_type=jnp.float32)
    ffn_hidden = (jax.nn.gelu(gate_pre) * up_pre).astype(jnp.bfloat16)
    ffn_out = jnp.einsum('stgf,gfd->std', ffn_hidden, down, preferred_element_type=jnp.float32)
    return (hidden.astype(jnp.float32) + ffn_out).astype(jnp.bfloat16)


def moe_kernel(tp, ep, ff_tile, sent_ref, w_in_ref, w_out_ref, keys_ref, values_ref, back_ref, keys_out_ref, values_out_ref, turn_ref, relay_kv_ref, stage_ref, rows_ref, result_ref, relay_y_ref, relay_x_ref,
               in_slots, out_slots, send_sem, recv_sem, weight_sem, local_sem):
    me_tp, me_ep = lax.axis_index('tp'), lax.axis_index('ep')
    right, left, across = lax.rem(me_tp + 1, tp), lax.rem(me_tp + tp - 1, tp), lax.rem(me_tp + 2, tp)

    def partner_of(index):
        return index + 1 - 2 * lax.rem(index, 2)

    partner = partner_of(me_ep)
    east, west, beyond = lax.rem(me_ep + 2, ep), lax.rem(me_ep + ep - 2, ep), lax.rem(me_ep + 4, ep)
    east_other, west_other, beyond_other = partner_of(east), partner_of(west), partner_of(beyond)
    peers = [{'tp': right}, {'tp': left}] + [{'ep': index} for index in (partner, east, east_other, west, west_other)]
    to_right, to_left = peers[:2]

    barrier = pltpu.get_barrier_semaphore()
    for peer in peers:
        pl.semaphore_signal(barrier, inc=1, device_id=peer, device_id_type=MESH)
    pl.semaphore_wait(barrier, len(peers))

    experts = w_in_ref.shape[0]
    half_y, half_x = ep // 2, tp // 2
    copies, local_copies = [], []

    def send(source, target, peer):
        index = len(copies)
        copy = pltpu.make_async_remote_copy(src_ref=source, dst_ref=target, send_sem=send_sem.at[index], recv_sem=recv_sem.at[index],
                                            device_id=peer, device_id_type=MESH)
        copy.start()
        copies.append(copy)
        return copy

    def keep(source, target):
        copy = pltpu.make_async_copy(source, target, local_sem.at[len(local_copies)])
        copy.start()
        local_copies.append(copy)
        return copy

    def fetch(expert):
        slot = expert % 2
        pair = (pltpu.make_async_copy(w_in_ref.at[expert], in_slots.at[slot], weight_sem.at[slot, 0]),
                pltpu.make_async_copy(w_out_ref.at[expert], out_slots.at[slot], weight_sem.at[slot, 1]))
        for copy in pair:
            copy.start()
        return pair

    class Exchange:
        def __init__(self, way, expert, source, middle, target):
            self.source, self.middle, self.target = source, middle, target
            self.relay_y, self.relay_x = relay_y_ref.at[way, expert], relay_x_ref.at[way, expert]

        def start_y(self):
            self.hops = [send(self.source(across).at[0:half_y], self.relay_y.at[0], to_right),
                         send(self.source(across).at[half_y:ep], self.relay_y.at[1], to_left)]
            self.direct = [send(self.source(right), self.middle.at[me_tp], to_right), send(self.source(left), self.middle.at[me_tp], to_left)]
            self.own = keep(self.source(me_tp), self.middle.at[me_tp])

        def forward_y(self):
            self.hops[0].wait_recv()
            self.direct.append(send(self.relay_y.at[0], self.middle.at[left, 0:half_y], to_right))
            self.hops[1].wait_recv()
            self.direct.append(send(self.relay_y.at[1], self.middle.at[right, half_y:ep], to_left))

        def finish_y(self):
            for copy in self.direct:
                copy.wait_recv()
            self.own.wait()

        def start_x(self):
            self.hops, self.direct = [], []
            for way, (near, low, high) in enumerate(((east, 0, half_x), (west, half_x, tp))):
                for index, far in enumerate((beyond, beyond_other)):
                    self.hops.append(send(self.middle.at[low:high, far], self.relay_x.at[way, index], {'ep': near}))
            for near in (east, west, east_other, west_other, partner):
                self.direct.append(send(self.middle.at[:, near], self.target(me_ep), {'ep': near}))

        def forward_x(self):
            for way, (origin, low, high, ends) in enumerate(((west, 0, half_x, (east, east_other)), (east, half_x, tp, (west, west_other)))):
                for index, end in enumerate(ends):
                    self.hops[2 * way + index].wait_recv()
                    self.direct.append(send(self.relay_x.at[way, index], self.target(origin).at[low:high], {'ep': end}))

        def finish_x(self):
            for copy in self.direct:
                copy.wait_recv()

    def outward(expert):
        return Exchange(0, expert, lambda index: sent_ref.at[index, :, expert], stage_ref.at[expert],
                        lambda index: rows_ref.at[expert, :, index])

    def inward(expert):
        return Exchange(1, expert, lambda index: result_ref.at[expert, index], turn_ref.at[expert],
                        lambda index: back_ref.at[:, index, expert])

    def compute(expert, begin, end):
        slot = expert % 2
        if begin == 0:
            for copy in weights[expert]:
                copy.wait()
            rows_ref[expert, :, me_ep] = stage_ref[expert, :, me_ep]
        row_shape = rows_ref.shape[2:]
        d_model, ff_dim = w_in_ref.shape[1:]

        def one_tile(tile, carry):
            rows = rows_ref[expert, tile].reshape(row_shape[0] * row_shape[1], row_shape[2])
            total = None
            for start in range(0, ff_dim, ff_tile):
                pre = jnp.dot(rows, in_slots[slot, :, start:start + ff_tile], preferred_element_type=jnp.float32)
                act = jax.nn.gelu(pre).astype(jnp.bfloat16)
                part = jnp.dot(act, out_slots[slot, start:start + ff_tile], preferred_element_type=jnp.float32)
                total = part if total is None else total + part
            result_ref[expert, tile] = total.astype(jnp.bfloat16).reshape(row_shape)
            return carry

        lax.fori_loop(begin, end, one_tile, 0)

    out = [outward(expert) for expert in range(experts)]
    ret = [inward(expert) for expert in range(experts)]
    chain = out + ret
    weights = {}
    last = len(chain) - 1
    chain[0].start_y()
    weights[0] = fetch(0)
    weights[1] = fetch(1)
    for step in range(last + 2):
        expert = step - 2
        if 0 <= expert < experts:
            compute(expert, 0, 1)
        if step <= last:
            chain[step].forward_y()
            if step < last:
                chain[step + 1].start_y()
        if step >= 1:
            chain[step - 1].forward_x()
        if 0 <= expert < experts:
            compute(expert, 1, tp)
            if expert + 2 < experts:
                weights[expert + 2] = fetch(expert + 2)
        if step <= last:
            chain[step].finish_y()
            chain[step].start_x()
        if 1 <= step <= experts:
            out[step - 1].finish_x()
        if step == last - 1:
            near_seqs = keys_ref.shape[1] // 2
            spans = (slice(0, near_seqs), slice(near_seqs, 2 * near_seqs))
            pairs = ((keys_ref, keys_out_ref), (values_ref, values_out_ref))
            cache_own = [keep(source.at[me_tp], target.at[me_tp]) for source, target in pairs]
        if step == last:
            cache_hops = [send(source.at[across, spans[way]], relay_kv_ref.at[index, way], peer)
                          for index, (source, _) in enumerate(pairs) for way, peer in enumerate((to_right, to_left))]
            cache_moves = [send(source.at[goal], target.at[me_tp], peer)
                           for source, target in pairs for goal, peer in ((right, to_right), (left, to_left))]
    own = [keep(turn_ref.at[expert, :, me_ep], back_ref.at[:, me_ep, expert]) for expert in range(experts)]
    for index, (_, target) in enumerate(pairs):
        for way, (origin, peer) in enumerate(((left, to_right), (right, to_left))):
            cache_hops[2 * index + way].wait_recv()
            cache_moves.append(send(relay_kv_ref.at[index, way], target.at[origin, spans[way]], peer))
    for exchange in ret:
        exchange.finish_x()
    for copy in cache_moves:
        copy.wait_recv()
    for copy in cache_own:
        copy.wait()
    for copy in own:
        copy.wait()
    for copy in copies:
        copy.wait_send()


def moe_exchange(dispatched, expert_in, expert_out, keys, values, tp, ep):
    experts, d_model, ff_dim = expert_in.shape
    slots = dispatched.shape[0] // (tp * ep * experts)
    view = dispatched.reshape(tp, ep, experts, slots, d_model)
    any_spec = pl.BlockSpec(memory_space=pl.ANY)
    rows = (experts, tp, ep, slots, d_model)
    count = experts * 2 * (6 + 13) + 12
    cache = jax.ShapeDtypeStruct(keys.shape, keys.dtype)
    relay = jax.ShapeDtypeStruct((2, 2, keys.shape[1] // 2) + keys.shape[2:], keys.dtype)
    dtype = dispatched.dtype
    total_rows = dispatched.shape[0]
    back, keys, values, _, _ = pl.pallas_call(
        functools.partial(moe_kernel, tp, ep, ff_dim // 4),
        in_specs=[any_spec] * 5,
        out_specs=[any_spec] * 5,
        out_shape=[jax.ShapeDtypeStruct(view.shape, dtype), cache, cache, jax.ShapeDtypeStruct(rows, dtype), relay],
        scratch_shapes=[pltpu.VMEM(rows, dtype), pltpu.VMEM(rows, dtype), pltpu.VMEM(rows, dtype),
                        pltpu.VMEM((2, experts, 2, ep // 2, slots, d_model), dtype), pltpu.VMEM((2, experts, 2, 2, tp // 2, slots, d_model), dtype),
                        pltpu.VMEM((2, d_model, ff_dim), dtype), pltpu.VMEM((2, ff_dim, d_model), dtype),
                        pltpu.SemaphoreType.DMA((count,)), pltpu.SemaphoreType.DMA((count,)), pltpu.SemaphoreType.DMA((2, 2)),
                        pltpu.SemaphoreType.DMA((3 * experts + 2,))],
        compiler_params=pltpu.CompilerParams(collective_id=1, has_side_effects=True, vmem_limit_bytes=62 * 1024 * 1024),
        cost_estimate=pl.CostEstimate(flops=4 * total_rows * d_model * ff_dim, bytes_accessed=4 * expert_in.size, transcendentals=0),
        name='moe_exchange',
    )(view, expert_in, expert_out, keys, values)
    return back.reshape(dispatched.shape), keys, values


def dispatch_kernel(hidden_ref, ln_ref, ids_ref, out_ref, normed_ref):
    @pl.when(pl.program_id(0) == 0)
    def _():
        rows = hidden_ref[...].astype(jnp.float32)
        inv_rms = lax.rsqrt(jnp.mean(rows * rows, axis=-1, keepdims=True) + EPSILON)
        normed_ref[...] = (rows * inv_rms * ln_ref[...]).astype(jnp.bfloat16)

    slots = lax.broadcasted_iota(jnp.int32, (out_ref.shape[0], hidden_ref.shape[0]), 0) + pl.program_id(0) * out_ref.shape[0]
    hit = (ids_ref[0:1] == slots) | (ids_ref[1:2] == slots)
    select = jnp.where(hit, 1.0, 0.0).astype(jnp.bfloat16)
    out_ref[...] = jnp.dot(select, normed_ref[...], preferred_element_type=jnp.float32).astype(jnp.bfloat16)


def dispatch(rows, ln_scale, slot_ids, num_slots):
    tokens, d_model = rows.shape
    block = num_slots // 8
    return pl.pallas_call(
        dispatch_kernel,
        grid=(num_slots // block,),
        in_specs=[pl.BlockSpec((tokens, d_model), lambda s: (0, 0)), pl.BlockSpec((1, d_model), lambda s: (0, 0)),
                  pl.BlockSpec((2, tokens), lambda s: (0, 0))],
        out_specs=pl.BlockSpec((block, d_model), lambda s: (s, 0)),
        out_shape=jax.ShapeDtypeStruct((num_slots, d_model), jnp.bfloat16),
        scratch_shapes=[pltpu.VMEM((tokens, d_model), jnp.bfloat16)],
        compiler_params=pltpu.CompilerParams(dimension_semantics=('arbitrary',), vmem_limit_bytes=32 * 1024 * 1024),
        cost_estimate=pl.CostEstimate(flops=2 * tokens * num_slots * d_model, bytes_accessed=2 * num_slots * d_model, transcendentals=0),
        name='dispatch',
    )(rows, ln_scale[None], jnp.swapaxes(slot_ids, 0, 1))


def slot_table(choices, num_experts):
    experts = jnp.arange(num_experts, dtype=jnp.int32)
    first_hot = (choices[..., 0:1] == experts).astype(jnp.int32)
    second_hot = (choices[..., 1:2] == experts).astype(jnp.int32)
    first_pos = jnp.sum((jnp.cumsum(first_hot, axis=-2) - 1) * first_hot, axis=-1)
    second_base = jnp.cumsum(second_hot, axis=-2) - 1 + jnp.sum(first_hot, axis=-2, keepdims=True)
    second_pos = jnp.sum(second_base * second_hot, axis=-1)
    return jnp.stack([first_pos, second_pos], axis=-1)


def moe_block(hidden, ln_scale, w_router, expert_in, expert_out, expert_ids, caches, tp, ep):
    local_batch, local_seq, d_model = hidden.shape
    tokens = local_batch * local_seq
    num_experts = w_router.shape[1]
    capacity = 4 * tokens // num_experts
    choices = expert_ids.reshape(tokens, 2)
    position = slot_table(choices, num_experts)
    slot_ids = jnp.where(position < capacity, choices * capacity + position, -1)
    columns = jnp.arange(num_experts * capacity, dtype=jnp.int32)
    select = (slot_ids[:, :, None] == columns).astype(jnp.bfloat16)

    normed = rms_norm(hidden, ln_scale).reshape(tokens, d_model)
    dispatched = dispatch(hidden.reshape(tokens, d_model), ln_scale, slot_ids, num_experts * capacity)
    returned, *caches = moe_exchange(dispatched, expert_in, expert_out, *caches, tp, ep)

    logits = jnp.dot(normed.astype(jnp.float32), w_router, precision=lax.Precision.HIGHEST)
    router_probs = jax.nn.softmax(logits, axis=-1)
    experts = jnp.arange(num_experts, dtype=jnp.int32)
    picked = jnp.sum(jnp.where(choices[:, :, None] == experts, router_probs[:, None, :], 0.0), axis=-1)
    gate_weights = picked / jnp.sum(picked, axis=-1, keepdims=True)

    gathered_out = jnp.einsum('ncs,sd->ncd', select, returned, preferred_element_type=jnp.float32)
    moe_sum = jnp.sum(gate_weights[:, :, None] * gathered_out, axis=1).reshape(local_batch, local_seq, d_model)
    return (hidden.astype(jnp.float32) + moe_sum).astype(jnp.bfloat16), *caches


def solution(mesh):
    tp, ep = mesh.shape['tp'], mesh.shape['ep']
    act_spec = P(('dp', 'ep'), 'tp', None)
    col_spec = P(None, None, 'tp')
    row_spec = P(None, 'tp', None)
    expert_spec = P(('tp', 'ep'), None, None)
    cache_spec = P(None, ('dp', 'ep'), 'tp', None, None)
    in_specs = (act_spec, P(), P(), col_spec, col_spec, col_spec, row_spec, row_spec,
                P(None, 'tp'), P(None, 'tp'), P('tp', None), P(), expert_spec, expert_spec, act_spec)

    def as_cache(got, local_heads):
        return jnp.swapaxes(got.reshape(got.shape[0] * got.shape[1], local_heads, -1, got.shape[3]), 2, 3)

    def device_fn(hidden_in, ln_attn, ln_ffn, w_query, w_key, w_value, w_out, bias_table, w_gate, w_up, w_down, w_router, expert_in, expert_out, expert_ids):
        def packed(layer):
            parts = [jnp.swapaxes(w[layer], 0, 1) for w in (w_query, w_key, w_value)] + [w_out[layer]]
            return jnp.concatenate(parts, axis=0)

        local_heads = bias_table.shape[1]
        blocks = [packed(0), w_up, w_down, packed(1), w_gate]
        hidden, tables, (attn_zero, up, down, attn_one, gate) = gather_all(hidden_in, bias_table, blocks, len(blocks) - 1, tp, ep)
        hidden, keys_zero, values_zero = attention(hidden, ln_attn[0], attn_zero, tables[0], tp)
        hidden = dense_ffn(hidden, ln_ffn[0], gate, up, down)
        hidden, keys_one, values_one, keys_zero, values_zero = attention(hidden, ln_attn[1], attn_one, tables[1], tp, (keys_zero, values_zero))
        hidden = lax.all_to_all(hidden, 'tp', 1, 0, tiled=True)
        hidden, keys_one, values_one = moe_block(hidden, ln_ffn[1], w_router, expert_in, expert_out, expert_ids, (keys_one, values_one), tp, ep)
        keys = jnp.stack([as_cache(keys_zero, local_heads), as_cache(keys_one, local_heads)])
        values = jnp.stack([as_cache(values_zero, local_heads), as_cache(values_one, local_heads)])
        return hidden, keys, values

    return jax.shard_map(device_fn, mesh=mesh, in_specs=in_specs, out_specs=(act_spec, cache_spec, cache_spec), check_vma=False)
```

```python
import functools

import jax
import jax.numpy as jnp
from jax import lax
from jax.experimental import pallas as pl
from jax.experimental.pallas import tpu as pltpu
from jax.sharding import PartitionSpec as P

EXACT_BUCKETS = 16
THRESHOLDS = (18, 20, 23, 26, 30, 34, 39, 45, 51, 58, 66, 76, 86, 98, 112)
EPSILON = 1e-6
GROUP = ('tp', 'ep')
MESH = pl.DeviceIdType.MESH


def rms_norm(rows_in, ln_scale):
    wide_rows = rows_in.astype(jnp.float32)
    inv_rms = lax.rsqrt(jnp.mean(wide_rows * wide_rows, axis=-1, keepdims=True) + EPSILON)
    return (wide_rows * inv_rms * ln_scale).astype(jnp.bfloat16)


def gather_kernel(tp, ep, num_blocks, direct, hidden_ref, table_ref, *refs):
    sources, refs = refs[:num_blocks], refs[num_blocks:]
    seqs_ref, relay_ref, tables_ref, refs = refs[0], refs[1], refs[2], refs[3:]
    gathered, refs = refs[:num_blocks], refs[num_blocks:]
    stage_ref, stage_hidden_ref, send_sem, recv_sem, in_sem, out_sem = refs
    me_tp, me_ep = lax.axis_index('tp'), lax.axis_index('ep')
    right, left, across = lax.rem(me_tp + 1, tp), lax.rem(me_tp + tp - 1, tp), lax.rem(me_tp + 2, tp)
    east, west, beyond = lax.rem(me_ep + 2, ep), lax.rem(me_ep + ep - 2, ep), lax.rem(me_ep + 4, ep)
    partner = me_ep + 1 - 2 * lax.rem(me_ep, 2)
    peers = ({'tp': right}, {'tp': left}, {'tp': across}, {'ep': east}, {'ep': west}, {'ep': partner})
    to_right, to_left, to_across, to_east, to_west, to_partner = peers

    barrier = pltpu.get_barrier_semaphore()
    for peer in peers:
        pl.semaphore_signal(barrier, inc=1, device_id=peer, device_id_type=MESH)
    pl.semaphore_wait(barrier, len(peers))

    copies = []

    def send(source, target, peer):
        index = len(copies)
        copy = pltpu.make_async_remote_copy(src_ref=source, dst_ref=target, send_sem=send_sem.at[index], recv_sem=recv_sem.at[index],
                                            device_id=peer, device_id_type=MESH)
        copy.start()
        copies.append(copy)
        return copy

    rows = sources[0].shape[1]
    halves = (slice(0, rows // 2), slice(rows // 2, rows))
    sliced = [block for block in range(num_blocks) if block != direct]
    locals_in = [pltpu.make_async_copy(sources[block], stage_ref.at[block], in_sem.at[block]) for block in range(num_blocks)]
    locals_in.append(pltpu.make_async_copy(hidden_ref.at[me_tp], stage_hidden_ref, in_sem.at[num_blocks]))

    first = {}
    for block in sliced:
        first[block] = [send(sources[block].at[me_ep], gathered[block].at[me_tp, me_ep], peer) for peer in (to_right, to_left)]
    tables = [send(table_ref, tables_ref.at[me_tp], peer) for peer in (to_right, to_left, to_across)]
    for copy in locals_in:
        copy.start()
    tables_ref[me_tp] = table_ref[...]
    part = hidden_ref.shape[1] // 2
    relays = [send(hidden_ref.at[across, 0:part], relay_ref.at[0], to_right), send(hidden_ref.at[across, part:2 * part], relay_ref.at[1], to_left)]

    def share(block, group, index, span=None):
        ref = gathered[block]
        return ref.at[group, index] if span is None else ref.at[group, index, span]

    received = []
    forward, sideways = {}, {}
    for block in sliced:
        first[block][0].wait_recv()
        forward[block] = [send(share(block, left, me_ep, halves[0]), share(block, left, me_ep, halves[0]), to_right)]
        sideways[block] = {}
        for group, name in ((left, 'left'), (right, 'right')):
            if name == 'right':
                first[block][1].wait_recv()
                forward[block].append(send(share(block, right, me_ep, halves[1]), share(block, right, me_ep, halves[1]), to_left))
            whole = share(block, group, me_ep)
            sideways[block][name] = [send(whole, whole, to_east), send(whole, whole, to_west)]
            received.append(send(whole, whole, to_partner))
    core_half = ep // 2
    base = lax.rem(me_ep, 2) * core_half
    near = pl.ds(base, core_half)
    direct_first = [send(sources[direct].at[near], gathered[direct].at[me_tp, near], peer) for peer in (to_right, to_left)]
    swaps = [send(hidden_ref.at[right], seqs_ref.at[:, me_tp], to_right), send(hidden_ref.at[left], seqs_ref.at[:, me_tp], to_left)]
    for block in sliced:
        for copy in forward[block]:
            copy.wait_recv()
        whole = share(block, across, me_ep)
        sideways[block]['across'] = [send(whole, whole, to_east), send(whole, whole, to_west)]
        received.append(send(whole, whole, to_partner))
    for copy in relays:
        copy.wait_recv()
    swaps.append(send(relay_ref.at[0], seqs_ref.at[0:part, left], to_right))
    swaps.append(send(relay_ref.at[1], seqs_ref.at[part:2 * part, right], to_left))
    for copy in locals_in:
        copy.wait()
    locals_out = [pltpu.make_async_copy(stage_ref.at[block], gathered[block].at[me_tp], out_sem.at[block]) for block in range(num_blocks)]
    locals_out.append(pltpu.make_async_copy(stage_hidden_ref, seqs_ref.at[:, me_tp], out_sem.at[num_blocks]))
    for copy in locals_out:
        copy.start()

    def direct_ring():
        for copy in direct_first:
            copy.wait_recv()
        lower, upper = pl.ds(base, core_half // 2), pl.ds(base + core_half // 2, core_half // 2)
        last = [send(gathered[direct].at[left, lower], gathered[direct].at[left, lower], to_right),
                send(gathered[direct].at[right, upper], gathered[direct].at[right, upper], to_left)]
        for group in (left, right):
            received.append(send(gathered[direct].at[group, near], gathered[direct].at[group, near], to_partner))
        return last

    direct_last = None
    final = []
    groups = {'left': left, 'right': right, 'across': across}
    for count, block in enumerate(sliced):
        for name in ('left', 'right', 'across'):
            group = groups[name]
            sideways[block][name][0].wait_recv()
            pair = [send(share(block, group, west, halves[0]), share(block, group, west, halves[0]), to_east)]
            whole = share(block, group, west)
            received.append(send(whole, whole, to_partner))
            sideways[block][name][1].wait_recv()
            pair.append(send(share(block, group, east, halves[1]), share(block, group, east, halves[1]), to_west))
            whole = share(block, group, east)
            received.append(send(whole, whole, to_partner))
            final.append((block, group, pair))
        if count == 1:
            direct_last = direct_ring()
    for block, group, pair in final:
        for copy in pair:
            copy.wait_recv()
        whole = share(block, group, beyond)
        received.append(send(whole, whole, to_partner))
    for copy in direct_last:
        copy.wait_recv()
    whole = gathered[direct].at[across, near]
    received.append(send(whole, whole, to_partner))
    for copy in tables + swaps + received:
        copy.wait_recv()
    for copy in copies:
        copy.wait_send()
    for copy in locals_out:
        copy.wait()


def gather_all(hidden_in, table, blocks, direct, tp, ep):
    num_blocks = len(blocks)
    batch, local_seq, d_model = hidden_in.shape
    seqs = batch // tp
    hidden_view = hidden_in.reshape(tp, seqs, local_seq, d_model)
    views = [block.reshape(ep, block.shape[0] // ep, block.shape[1]) for block in blocks]
    any_spec = pl.BlockSpec(memory_space=pl.ANY)
    vmem_spec = pl.BlockSpec(memory_space=pltpu.VMEM)
    copies = 28 * (num_blocks - 1) + 7 + 9
    results = pl.pallas_call(
        functools.partial(gather_kernel, tp, ep, num_blocks, direct),
        in_specs=[any_spec, vmem_spec] + [any_spec] * num_blocks,
        out_specs=[any_spec, any_spec, vmem_spec] + [any_spec] * num_blocks,
        out_shape=[jax.ShapeDtypeStruct((seqs, tp, local_seq, d_model), hidden_in.dtype),
                   jax.ShapeDtypeStruct((2, seqs // 2, local_seq, d_model), hidden_in.dtype),
                   jax.ShapeDtypeStruct((tp,) + table.shape, table.dtype)]
        + [jax.ShapeDtypeStruct((tp,) + view.shape, view.dtype) for view in views],
        scratch_shapes=[pltpu.VMEM((num_blocks,) + views[0].shape, views[0].dtype), pltpu.VMEM((seqs, local_seq, d_model), hidden_in.dtype),
                        pltpu.SemaphoreType.DMA((copies,)), pltpu.SemaphoreType.DMA((copies,)),
                        pltpu.SemaphoreType.DMA((num_blocks + 1,)), pltpu.SemaphoreType.DMA((num_blocks + 1,))],
        compiler_params=pltpu.CompilerParams(collective_id=0, has_side_effects=True),
        name='gather_all',
    )(hidden_view, table, *views)
    hidden = results[0].reshape(seqs, tp * local_seq, d_model)
    tables = jnp.swapaxes(results[2], 0, 1).reshape(table.shape[0], -1, table.shape[2])
    return hidden, tables, [block.reshape(tp, -1, d_model) for block in results[3:]]


def attention_kernel(tp, moving, hidden_ref, ln_ref, w_ref, table_ref, *refs):
    if moving:
        old_keys_ref, old_values_ref, out_ref, keys_ref, values_ref, new_keys_ref, new_values_ref = refs[:7]
        relay_ref, send_sem, recv_sem, local_sem = refs[12:]
        bias_ref, q_ref, kt_ref, ctx_ref, w_out_ref = refs[7:12]
    else:
        out_ref, keys_ref, values_ref, bias_ref, q_ref, kt_ref, ctx_ref, w_out_ref = refs
    seq_len, d_model = hidden_ref.shape[1], hidden_ref.shape[2]
    num_heads = table_ref.shape[0]
    head_dim = d_model // num_heads
    half = seq_len // 2
    width = d_model // tp
    starts = tuple(range(EXACT_BUCKETS + 1)) + THRESHOLDS

    if moving:
        me_tp = lax.axis_index('tp')
        right, left, across = lax.rem(me_tp + 1, tp), lax.rem(me_tp + tp - 1, tp), lax.rem(me_tp + 2, tp)
        pairs = ((old_keys_ref, new_keys_ref), (old_values_ref, new_values_ref))
        half_seqs = old_keys_ref.shape[1] // 2
        spans = (slice(0, half_seqs), slice(half_seqs, 2 * half_seqs))

        def remote(index, source, target, to):
            return pltpu.make_async_remote_copy(src_ref=source, dst_ref=target, send_sem=send_sem.at[index], recv_sem=recv_sem.at[index],
                                                device_id={'tp': to}, device_id_type=MESH)

        hops, directs, forwards, owns = [], [], [], []
        for index, (source, target) in enumerate(pairs):
            for way, (goal, origin) in enumerate(((right, left), (left, right))):
                number = 2 * index + way
                hops.append(remote(number, source.at[across, spans[way]], relay_ref.at[index, way], goal))
                directs.append(remote(4 + number, source.at[goal], target.at[me_tp], goal))
                forwards.append(remote(8 + number, relay_ref.at[index, way], target.at[origin, spans[way]], goal))
            owns.append(pltpu.make_async_copy(source.at[me_tp], target.at[me_tp], local_sem.at[index]))

        @pl.when(pl.program_id(0) == 0)
        def _():
            barrier = pltpu.get_barrier_semaphore()
            for goal in (right, left):
                pl.semaphore_signal(barrier, inc=1, device_id={'tp': goal}, device_id_type=MESH)
            pl.semaphore_wait(barrier, 2)
            for copy in hops + directs + owns:
                copy.start()

        @pl.when(pl.program_id(0) == 2)
        def _():
            for hop, forward in zip(hops, forwards):
                hop.wait_recv()
                forward.start()

    @pl.when(pl.program_id(0) == 0)
    def _():
        def one_head(head, carry):
            for block in range(2):
                key_pos = lax.broadcasted_iota(jnp.int32, (half, half), 0)
                query_pos = lax.broadcasted_iota(jnp.int32, (half, half), 1) + block * half
                rel_pos = query_pos - key_pos
                bias = jnp.full((half, half), -jnp.inf, jnp.float32)
                for bucket, start in enumerate(starts):
                    bias = jnp.where(rel_pos >= start, table_ref[head, bucket], bias)
                bias_ref[head, :, block * half:(block + 1) * half] = bias
            return carry

        lax.fori_loop(0, num_heads, one_head, 0)
        for part in range(tp):
            w_out_ref[part * width:(part + 1) * width] = w_ref[part, 3 * width:]

    rows = hidden_ref[0].astype(jnp.float32)
    inv_rms = lax.rsqrt(jnp.mean(rows * rows, axis=-1, keepdims=True) + EPSILON)
    normed = (rows * inv_rms * ln_ref[...]).astype(jnp.bfloat16)
    nt = (((1,), (1,)), ((), ()))
    for part in range(tp):
        take = slice(part * width, (part + 1) * width)
        qkv = lax.dot_general(w_ref[part, :3 * width], normed, nt, preferred_element_type=jnp.float32).astype(jnp.bfloat16)
        q_ref[take] = qkv[:width]
        keys_ref[part, 0] = qkv[width:2 * width]
        values_ref[part, 0] = qkv[2 * width:]
        kt_ref[take] = qkv[width:2 * width]

    local_heads = num_heads // tp
    zeros = jnp.zeros((head_dim, seq_len), jnp.bfloat16)
    for head in range(num_heads):
        pair = slice((head // 2) * 2 * head_dim, (head // 2 + 1) * 2 * head_dim)
        q_head = q_ref[head * head_dim:(head + 1) * head_dim]
        q_pair = jnp.concatenate([q_head, zeros] if head % 2 == 0 else [zeros, q_head], axis=0)
        scores = jnp.dot(kt_ref[pair].T, q_pair, preferred_element_type=jnp.float32)
        value = values_ref[head // local_heads, 0, (head % local_heads) * head_dim:(head % local_heads + 1) * head_dim]
        near, far = bias_ref[head, :, :half], bias_ref[head, :, half:]
        scale = head_dim ** -0.5
        first = scores[:half, :half] * scale + near
        first = jnp.exp(first - jnp.max(first, axis=0, keepdims=True))
        probs = (first / jnp.sum(first, axis=0, keepdims=True)).astype(jnp.bfloat16)
        ctx_first = jnp.dot(value[:, :half], probs, preferred_element_type=jnp.float32)
        low = scores[:half, half:] * scale + far
        high = scores[half:, half:] * scale + near
        top = jnp.maximum(jnp.max(low, axis=0, keepdims=True), jnp.max(high, axis=0, keepdims=True))
        low, high = jnp.exp(low - top), jnp.exp(high - top)
        total = jnp.sum(low, axis=0, keepdims=True) + jnp.sum(high, axis=0, keepdims=True)
        probs = jnp.concatenate([(low / total).astype(jnp.bfloat16), (high / total).astype(jnp.bfloat16)], axis=0)
        ctx_second = jnp.dot(value, probs, preferred_element_type=jnp.float32)
        ctx = jnp.concatenate([ctx_first, ctx_second], axis=1)
        ctx_ref[head * head_dim:(head + 1) * head_dim] = ctx.astype(jnp.bfloat16)
    attn_out = jnp.dot(ctx_ref[...].T, w_out_ref[...], preferred_element_type=jnp.float32)
    out_ref[0] = (rows + attn_out).astype(jnp.bfloat16)

    if moving:
        @pl.when(pl.program_id(0) == pl.num_programs(0) - 1)
        def _():
            for copy in directs + forwards:
                copy.wait_recv()
            for copy in hops + directs + forwards:
                copy.wait_send()
            for copy in owns:
                copy.wait()


def attention(hidden, ln_scale, packed, table, tp, old=()):
    seqs, seq_len, d_model = hidden.shape
    num_heads = table.shape[0]
    width = d_model // tp
    seq_block = pl.BlockSpec((1, seq_len, d_model), lambda s: (s, 0, 0))
    cache_block = pl.BlockSpec((tp, 1, width, seq_len), lambda s: (0, s, 0, 0))
    cache = jax.ShapeDtypeStruct((tp, seqs, width, seq_len), jnp.bfloat16)
    flops = 2 * seqs * seq_len * d_model * (5 * d_model + 3 * seq_len)
    any_spec = pl.BlockSpec(memory_space=pl.ANY)
    scratch = [pltpu.VMEM((num_heads, seq_len // 2, seq_len), jnp.float32), pltpu.VMEM((d_model, seq_len), jnp.bfloat16),
               pltpu.VMEM((d_model, seq_len), jnp.bfloat16), pltpu.VMEM((d_model, seq_len), jnp.bfloat16),
               pltpu.VMEM((d_model, d_model), jnp.bfloat16)]
    options = {}
    if old:
        scratch += [pltpu.VMEM((2, 2, seqs // 2) + cache.shape[2:], jnp.bfloat16), pltpu.SemaphoreType.DMA((12,)),
                    pltpu.SemaphoreType.DMA((12,)), pltpu.SemaphoreType.DMA((2,))]
        options = dict(collective_id=2, has_side_effects=True)
    return pl.pallas_call(
        functools.partial(attention_kernel, tp, bool(old)),
        grid=(seqs,),
        in_specs=[seq_block, pl.BlockSpec((1, d_model), lambda s: (0, 0)), pl.BlockSpec((tp, d_model, d_model), lambda s: (0, 0, 0)),
                  pl.BlockSpec(memory_space=pltpu.SMEM)] + [any_spec] * len(old),
        out_specs=[seq_block, cache_block, cache_block] + [any_spec] * len(old),
        out_shape=[jax.ShapeDtypeStruct(hidden.shape, hidden.dtype), cache, cache] + [cache] * len(old),
        scratch_shapes=scratch,
        compiler_params=pltpu.CompilerParams(dimension_semantics=('arbitrary',), vmem_limit_bytes=40 * 1024 * 1024, **options),
        cost_estimate=pl.CostEstimate(flops=flops, bytes_accessed=2 * (hidden.size * 4 + packed.size), transcendentals=0),
        name='attention_moving' if old else 'attention',
    )(hidden, ln_scale[None], packed, table, *old)


def dense_ffn(hidden, ln_scale, gate, up, down):
    normed = rms_norm(hidden, ln_scale)
    gate_pre = jnp.einsum('std,gdf->stgf', normed, gate, preferred_element_type=jnp.float32)
    up_pre = jnp.einsum('std,gdf->stgf', normed, up, preferred_element_type=jnp.float32)
    ffn_hidden = (jax.nn.gelu(gate_pre) * up_pre).astype(jnp.bfloat16)
    ffn_out = jnp.einsum('stgf,gfd->std', ffn_hidden, down, preferred_element_type=jnp.float32)
    return (hidden.astype(jnp.float32) + ffn_out).astype(jnp.bfloat16)


def moe_kernel(tp, ep, ff_tile, sent_ref, w_in_ref, w_out_ref, keys_ref, values_ref, back_ref, keys_out_ref, values_out_ref, turn_ref, relay_kv_ref, stage_ref, rows_ref, result_ref, relay_y_ref, relay_x_ref,
               in_slots, out_slots, send_sem, recv_sem, weight_sem, local_sem):
    me_tp, me_ep = lax.axis_index('tp'), lax.axis_index('ep')
    right, left, across = lax.rem(me_tp + 1, tp), lax.rem(me_tp + tp - 1, tp), lax.rem(me_tp + 2, tp)

    def partner_of(index):
        return index + 1 - 2 * lax.rem(index, 2)

    partner = partner_of(me_ep)
    east, west, beyond = lax.rem(me_ep + 2, ep), lax.rem(me_ep + ep - 2, ep), lax.rem(me_ep + 4, ep)
    east_other, west_other, beyond_other = partner_of(east), partner_of(west), partner_of(beyond)
    peers = [{'tp': right}, {'tp': left}] + [{'ep': index} for index in (partner, east, east_other, west, west_other)]
    to_right, to_left = peers[:2]

    barrier = pltpu.get_barrier_semaphore()
    for peer in peers:
        pl.semaphore_signal(barrier, inc=1, device_id=peer, device_id_type=MESH)
    pl.semaphore_wait(barrier, len(peers))

    experts = w_in_ref.shape[0]
    half_y, half_x = ep // 2, tp // 2
    copies, local_copies = [], []

    def send(source, target, peer):
        index = len(copies)
        copy = pltpu.make_async_remote_copy(src_ref=source, dst_ref=target, send_sem=send_sem.at[index], recv_sem=recv_sem.at[index],
                                            device_id=peer, device_id_type=MESH)
        copy.start()
        copies.append(copy)
        return copy

    def keep(source, target):
        copy = pltpu.make_async_copy(source, target, local_sem.at[len(local_copies)])
        copy.start()
        local_copies.append(copy)
        return copy

    def fetch(expert):
        slot = expert % 2
        pair = (pltpu.make_async_copy(w_in_ref.at[expert], in_slots.at[slot], weight_sem.at[slot, 0]),
                pltpu.make_async_copy(w_out_ref.at[expert], out_slots.at[slot], weight_sem.at[slot, 1]))
        for copy in pair:
            copy.start()
        return pair

    class Exchange:
        def __init__(self, way, expert, source, middle, target):
            self.source, self.middle, self.target = source, middle, target
            self.relay_y, self.relay_x = relay_y_ref.at[way, expert], relay_x_ref.at[way, expert]

        def start_y(self):
            self.hops = [send(self.source(across).at[0:half_y], self.relay_y.at[0], to_right),
                         send(self.source(across).at[half_y:ep], self.relay_y.at[1], to_left)]
            self.direct = [send(self.source(right), self.middle.at[me_tp], to_right), send(self.source(left), self.middle.at[me_tp], to_left)]
            self.own = keep(self.source(me_tp), self.middle.at[me_tp])

        def forward_y(self):
            self.hops[0].wait_recv()
            self.direct.append(send(self.relay_y.at[0], self.middle.at[left, 0:half_y], to_right))
            self.hops[1].wait_recv()
            self.direct.append(send(self.relay_y.at[1], self.middle.at[right, half_y:ep], to_left))

        def finish_y(self):
            for copy in self.direct:
                copy.wait_recv()
            self.own.wait()

        def start_x(self):
            self.hops, self.direct = [], []
            for way, (near, low, high) in enumerate(((east, 0, half_x), (west, half_x, tp))):
                for index, far in enumerate((beyond, beyond_other)):
                    self.hops.append(send(self.middle.at[low:high, far], self.relay_x.at[way, index], {'ep': near}))
            for near in (east, west, east_other, west_other, partner):
                self.direct.append(send(self.middle.at[:, near], self.target(me_ep), {'ep': near}))

        def forward_x(self):
            for way, (origin, low, high, ends) in enumerate(((west, 0, half_x, (east, east_other)), (east, half_x, tp, (west, west_other)))):
                for index, end in enumerate(ends):
                    self.hops[2 * way + index].wait_recv()
                    self.direct.append(send(self.relay_x.at[way, index], self.target(origin).at[low:high], {'ep': end}))

        def finish_x(self):
            for copy in self.direct:
                copy.wait_recv()

    def outward(expert):
        return Exchange(0, expert, lambda index: sent_ref.at[index, :, expert], stage_ref.at[expert],
                        lambda index: rows_ref.at[expert, :, index])

    def inward(expert):
        return Exchange(1, expert, lambda index: result_ref.at[expert, index], turn_ref.at[expert],
                        lambda index: back_ref.at[:, index, expert])

    def compute(expert, begin, end):
        slot = expert % 2
        if begin == 0:
            for copy in weights[expert]:
                copy.wait()
            rows_ref[expert, :, me_ep] = stage_ref[expert, :, me_ep]
        row_shape = rows_ref.shape[2:]
        d_model, ff_dim = w_in_ref.shape[1:]

        def one_tile(tile, carry):
            rows = rows_ref[expert, tile].reshape(row_shape[0] * row_shape[1], row_shape[2])
            total = None
            for start in range(0, ff_dim, ff_tile):
                pre = jnp.dot(rows, in_slots[slot, :, start:start + ff_tile], preferred_element_type=jnp.float32)
                act = jax.nn.gelu(pre).astype(jnp.bfloat16)
                part = jnp.dot(act, out_slots[slot, start:start + ff_tile], preferred_element_type=jnp.float32)
                total = part if total is None else total + part
            result_ref[expert, tile] = total.astype(jnp.bfloat16).reshape(row_shape)
            return carry

        lax.fori_loop(begin, end, one_tile, 0)

    out = [outward(expert) for expert in range(experts)]
    ret = [inward(expert) for expert in range(experts)]
    chain = out + ret
    weights, own = {}, []
    last = len(chain) - 1
    chain[0].start_y()
    weights[0] = fetch(0)
    weights[1] = fetch(1)
    for step in range(last + 2):
        expert = step - 2
        if 0 <= expert < experts:
            compute(expert, 0, 1)
        if step <= last:
            chain[step].forward_y()
            if step < last:
                chain[step + 1].start_y()
        if step >= 1:
            chain[step - 1].forward_x()
        if 0 <= expert < experts:
            compute(expert, 1, tp)
            if expert + 2 < experts:
                weights[expert + 2] = fetch(expert + 2)
        if step <= last:
            chain[step].finish_y()
            chain[step].start_x()
            if step >= experts:
                own.append(keep(turn_ref.at[step - experts, :, me_ep], back_ref.at[:, me_ep, step - experts]))
        if 1 <= step <= experts:
            out[step - 1].finish_x()
        if step == last - 1:
            near_seqs = keys_ref.shape[1] // 2
            spans = (slice(0, near_seqs), slice(near_seqs, 2 * near_seqs))
            pairs = ((keys_ref, keys_out_ref), (values_ref, values_out_ref))
            cache_own = [keep(source.at[me_tp], target.at[me_tp]) for source, target in pairs]
        if step == last:
            cache_hops = [send(source.at[across, spans[way]], relay_kv_ref.at[index, way], peer)
                          for index, (source, _) in enumerate(pairs) for way, peer in enumerate((to_right, to_left))]
            cache_moves = [send(source.at[goal], target.at[me_tp], peer)
                           for source, target in pairs for goal, peer in ((right, to_right), (left, to_left))]
    for index, (_, target) in enumerate(pairs):
        for way, (origin, peer) in enumerate(((left, to_right), (right, to_left))):
            cache_hops[2 * index + way].wait_recv()
            cache_moves.append(send(relay_kv_ref.at[index, way], target.at[origin, spans[way]], peer))
    for exchange in ret:
        exchange.finish_x()
    for copy in cache_moves:
        copy.wait_recv()
    for copy in cache_own:
        copy.wait()
    for copy in own:
        copy.wait()
    for copy in copies:
        copy.wait_send()


def moe_exchange(dispatched, expert_in, expert_out, keys, values, tp, ep):
    experts, d_model, ff_dim = expert_in.shape
    slots = dispatched.shape[0] // (tp * ep * experts)
    view = dispatched.reshape(tp, ep, experts, slots, d_model)
    any_spec = pl.BlockSpec(memory_space=pl.ANY)
    rows = (experts, tp, ep, slots, d_model)
    count = experts * 2 * (6 + 13) + 12
    cache = jax.ShapeDtypeStruct(keys.shape, keys.dtype)
    relay = jax.ShapeDtypeStruct((2, 2, keys.shape[1] // 2) + keys.shape[2:], keys.dtype)
    dtype = dispatched.dtype
    total_rows = dispatched.shape[0]
    back, keys, values, _, _ = pl.pallas_call(
        functools.partial(moe_kernel, tp, ep, ff_dim // 4),
        in_specs=[any_spec] * 5,
        out_specs=[any_spec] * 5,
        out_shape=[jax.ShapeDtypeStruct(view.shape, dtype), cache, cache, jax.ShapeDtypeStruct(rows, dtype), relay],
        scratch_shapes=[pltpu.VMEM(rows, dtype), pltpu.VMEM(rows, dtype), pltpu.VMEM(rows, dtype),
                        pltpu.VMEM((2, experts, 2, ep // 2, slots, d_model), dtype), pltpu.VMEM((2, experts, 2, 2, tp // 2, slots, d_model), dtype),
                        pltpu.VMEM((2, d_model, ff_dim), dtype), pltpu.VMEM((2, ff_dim, d_model), dtype),
                        pltpu.SemaphoreType.DMA((count,)), pltpu.SemaphoreType.DMA((count,)), pltpu.SemaphoreType.DMA((2, 2)),
                        pltpu.SemaphoreType.DMA((3 * experts + 2,))],
        compiler_params=pltpu.CompilerParams(collective_id=1, has_side_effects=True, vmem_limit_bytes=62 * 1024 * 1024),
        cost_estimate=pl.CostEstimate(flops=4 * total_rows * d_model * ff_dim, bytes_accessed=4 * expert_in.size, transcendentals=0),
        name='moe_exchange',
    )(view, expert_in, expert_out, keys, values)
    return back.reshape(dispatched.shape), keys, values


def dispatch_kernel(hidden_ref, ln_ref, ids_ref, out_ref, normed_ref):
    @pl.when(pl.program_id(0) == 0)
    def _():
        rows = hidden_ref[...].astype(jnp.float32)
        inv_rms = lax.rsqrt(jnp.mean(rows * rows, axis=-1, keepdims=True) + EPSILON)
        normed_ref[...] = (rows * inv_rms * ln_ref[...]).astype(jnp.bfloat16)

    slots = lax.broadcasted_iota(jnp.int32, (out_ref.shape[0], hidden_ref.shape[0]), 0) + pl.program_id(0) * out_ref.shape[0]
    hit = (ids_ref[0:1] == slots) | (ids_ref[1:2] == slots)
    select = jnp.where(hit, 1.0, 0.0).astype(jnp.bfloat16)
    out_ref[...] = jnp.dot(select, normed_ref[...], preferred_element_type=jnp.float32).astype(jnp.bfloat16)


def dispatch(rows, ln_scale, slot_ids, num_slots):
    tokens, d_model = rows.shape
    block = num_slots // 8
    return pl.pallas_call(
        dispatch_kernel,
        grid=(num_slots // block,),
        in_specs=[pl.BlockSpec((tokens, d_model), lambda s: (0, 0)), pl.BlockSpec((1, d_model), lambda s: (0, 0)),
                  pl.BlockSpec((2, tokens), lambda s: (0, 0))],
        out_specs=pl.BlockSpec((block, d_model), lambda s: (s, 0)),
        out_shape=jax.ShapeDtypeStruct((num_slots, d_model), jnp.bfloat16),
        scratch_shapes=[pltpu.VMEM((tokens, d_model), jnp.bfloat16)],
        compiler_params=pltpu.CompilerParams(dimension_semantics=('arbitrary',), vmem_limit_bytes=32 * 1024 * 1024),
        cost_estimate=pl.CostEstimate(flops=2 * tokens * num_slots * d_model, bytes_accessed=2 * num_slots * d_model, transcendentals=0),
        name='dispatch',
    )(rows, ln_scale[None], jnp.swapaxes(slot_ids, 0, 1))


def slot_table(choices, num_experts):
    experts = jnp.arange(num_experts, dtype=jnp.int32)
    first_hot = (choices[..., 0:1] == experts).astype(jnp.int32)
    second_hot = (choices[..., 1:2] == experts).astype(jnp.int32)
    first_pos = jnp.sum((jnp.cumsum(first_hot, axis=-2) - 1) * first_hot, axis=-1)
    second_base = jnp.cumsum(second_hot, axis=-2) - 1 + jnp.sum(first_hot, axis=-2, keepdims=True)
    second_pos = jnp.sum(second_base * second_hot, axis=-1)
    return jnp.stack([first_pos, second_pos], axis=-1)


def moe_block(hidden, ln_scale, w_router, expert_in, expert_out, expert_ids, caches, tp, ep):
    local_batch, local_seq, d_model = hidden.shape
    tokens = local_batch * local_seq
    num_experts = w_router.shape[1]
    capacity = 4 * tokens // num_experts
    choices = expert_ids.reshape(tokens, 2)
    position = slot_table(choices, num_experts)
    slot_ids = jnp.where(position < capacity, choices * capacity + position, -1)
    columns = jnp.arange(num_experts * capacity, dtype=jnp.int32)
    select = (slot_ids[:, :, None] == columns).astype(jnp.bfloat16)

    normed = rms_norm(hidden, ln_scale).reshape(tokens, d_model)
    dispatched = dispatch(hidden.reshape(tokens, d_model), ln_scale, slot_ids, num_experts * capacity)
    returned, *caches = moe_exchange(dispatched, expert_in, expert_out, *caches, tp, ep)

    logits = jnp.dot(normed.astype(jnp.float32), w_router, precision=lax.Precision.HIGHEST)
    router_probs = jax.nn.softmax(logits, axis=-1)
    experts = jnp.arange(num_experts, dtype=jnp.int32)
    picked = jnp.sum(jnp.where(choices[:, :, None] == experts, router_probs[:, None, :], 0.0), axis=-1)
    gate_weights = picked / jnp.sum(picked, axis=-1, keepdims=True)

    gathered_out = jnp.einsum('ncs,sd->ncd', select, returned, preferred_element_type=jnp.float32)
    moe_sum = jnp.sum(gate_weights[:, :, None] * gathered_out, axis=1).reshape(local_batch, local_seq, d_model)
    return (hidden.astype(jnp.float32) + moe_sum).astype(jnp.bfloat16), *caches


def solution(mesh):
    tp, ep = mesh.shape['tp'], mesh.shape['ep']
    act_spec = P(('dp', 'ep'), 'tp', None)
    col_spec = P(None, None, 'tp')
    row_spec = P(None, 'tp', None)
    expert_spec = P(('tp', 'ep'), None, None)
    cache_spec = P(None, ('dp', 'ep'), 'tp', None, None)
    in_specs = (act_spec, P(), P(), col_spec, col_spec, col_spec, row_spec, row_spec,
                P(None, 'tp'), P(None, 'tp'), P('tp', None), P(), expert_spec, expert_spec, act_spec)

    def as_cache(got, local_heads):
        return jnp.swapaxes(got.reshape(got.shape[0] * got.shape[1], local_heads, -1, got.shape[3]), 2, 3)

    def device_fn(hidden_in, ln_attn, ln_ffn, w_query, w_key, w_value, w_out, bias_table, w_gate, w_up, w_down, w_router, expert_in, expert_out, expert_ids):
        def packed(layer):
            parts = [jnp.swapaxes(w[layer], 0, 1) for w in (w_query, w_key, w_value)] + [w_out[layer]]
            return jnp.concatenate(parts, axis=0)

        local_heads = bias_table.shape[1]
        blocks = [packed(0), w_up, w_down, packed(1), w_gate]
        hidden, tables, (attn_zero, up, down, attn_one, gate) = gather_all(hidden_in, bias_table, blocks, len(blocks) - 1, tp, ep)
        hidden, keys_zero, values_zero = attention(hidden, ln_attn[0], attn_zero, tables[0], tp)
        hidden = dense_ffn(hidden, ln_ffn[0], gate, up, down)
        hidden, keys_one, values_one, keys_zero, values_zero = attention(hidden, ln_attn[1], attn_one, tables[1], tp, (keys_zero, values_zero))
        hidden = lax.all_to_all(hidden, 'tp', 1, 0, tiled=True)
        hidden, keys_one, values_one = moe_block(hidden, ln_ffn[1], w_router, expert_in, expert_out, expert_ids, (keys_one, values_one), tp, ep)
        keys = jnp.stack([as_cache(keys_zero, local_heads), as_cache(keys_one, local_heads)])
        values = jnp.stack([as_cache(values_zero, local_heads), as_cache(values_one, local_heads)])
        return hidden, keys, values

    return jax.shard_map(device_fn, mesh=mesh, in_specs=in_specs, out_specs=(act_spec, cache_spec, cache_spec), check_vma=False)
```
